32 devices in a mesh: lat: 4 (over z), lon: 4 (over y, x), lev: 2 (over core).
Axes of the slice: x: 2, y: 2, z: 4, core: 2. Of those that a mesh axis runs over, the one named last changes fastest.
Arguments:
- pressure: float32 [16, 256, 128, 128], P('lat', 'lon', 'lev'), may hold values from 0.2 to 1.8
- earlier: float32 [16, 256, 128, 128], P('lat', 'lon', 'lev'), may hold values from 0.2 to 1.8
- speed_square: float32 [16, 256, 128, 128], P('lat', 'lon', 'lev'), may hold values from 0.05 to 0.3
Outputs:
- pressure_end: float32 [16, 256, 128, 128], P('lat', 'lon', 'lev')
The draws below stay inside these ranges and needn't reach their ends.
All inputs are finite; a program needn't handle non-finite values.
Results may differ from the reference program's by a relative error of at most 0.00002.
Values sent between devices are 32-bit elements.
A program may use at most 320 MiB of HBM per device.

```python
import jax
import jax.numpy as jnp
from jax import lax

GRID_Y = 16
GRID_X = 256
GRID_Z = 128
LEVELS = 128
STEPS = 4


def block_levels(stream_key, extent, cuts, least, high):
    def one(dim, shards_of):
        steps = jax.random.uniform(jax.random.fold_in(jax.random.fold_in(stream_key, 6), dim), (shards_of,), jnp.float32, least / len(cuts), high / len(cuts))
        return jnp.repeat(jnp.exp(steps), extent[dim] // shards_of).reshape((-1,) + (1,) * (len(extent) - dim - 1))

    factor_of = one(*cuts[0])
    for cut in cuts[1:]:
        factor_of = factor_of * one(*cut)
    return factor_of


def setup_inputs(seed: int = 0) -> dict:
    splits = jax.random.split(jax.random.key(seed), 4)
    return {
        "pressure": jnp.clip(0.2 + 1.5999999 * jax.random.uniform(splits[0], (GRID_Y, GRID_X, GRID_Z, LEVELS), jnp.float32) ** block_levels(splits[0], (GRID_Y, GRID_X, GRID_Z, LEVELS), ((0, 4), (1, 4), (2, 2)), -0.2, 0.2), 0.2, 1.8),
        "earlier": jnp.clip(0.2 + 1.5999999 * jax.random.uniform(splits[1], (GRID_Y, GRID_X, GRID_Z, LEVELS), jnp.float32) ** block_levels(splits[1], (GRID_Y, GRID_X, GRID_Z, LEVELS), ((0, 4), (1, 4), (2, 2)), -0.2, 0.2), 0.2, 1.8),
        "speed_square": jnp.clip(0.05 + 0.25 * jax.random.uniform(splits[2], (GRID_Y, GRID_X, GRID_Z, LEVELS), jnp.float32) ** block_levels(splits[2], (GRID_Y, GRID_X, GRID_Z, LEVELS), ((0, 4), (1, 4), (2, 2)), -0.2, 0.2), 0.05, 0.3),
    }


def inner_cells(values, dims):
    for dim in dims:
        values = lax.slice_in_dim(values, 1, values.shape[dim] - 1, axis=dim)
    return values


def side_cells(values, dim, start, dims):
    others = [other for other in dims if other != dim]
    values = inner_cells(values, others)
    return lax.slice_in_dim(values, start, start + values.shape[dim] - 2, axis=dim)


def advance(padded, before, speed_square):
    middle = inner_cells(padded, (0, 1, 2))
    lower = [side_cells(padded, dim, 0, (0, 1, 2)) for dim in (0, 1, 2)]
    upper = [side_cells(padded, dim, 2, (0, 1, 2)) for dim in (0, 1, 2)]
    spread = lower[0] + upper[0] + lower[1] + upper[1] + lower[2] + upper[2] - 6.0 * middle
    return 2.0 * middle - before + speed_square * spread


def reference(pressure, earlier, speed_square):
    for step in range(STEPS):
        later = advance(jnp.pad(pressure, ((1, 1), (1, 1), (1, 1), (0, 0)), mode="constant"), earlier, speed_square)
        earlier, pressure = pressure, later
    return pressure
```

```python
import functools

import jax
import jax.numpy as jnp
from jax import lax
from jax.experimental import pallas as pl
from jax.experimental.pallas import tpu as pltpu
from jax.sharding import PartitionSpec as P

STEPS = 4
TAILS = (28, 8)
PAD = 8
AXES = ("lat", "lon", "lev")
MESH = pl.DeviceIdType.MESH


def late():
    return lax.axis_index("lev") % 2 == 0


def neighbours(counts):
    me = [lax.axis_index(axis) for axis in AXES]
    return me, [(place > 0, place < count - 1) for place, count in zip(me, counts)]


def greet(me, has, dims):
    barrier = pltpu.get_barrier_semaphore()
    greeted = jnp.int32(0)
    for dim in dims:
        for side, shift in enumerate((-1, 1)):
            greeted = greeted + has[dim][side].astype(jnp.int32)

            @pl.when(has[dim][side])
            def _():
                pl.semaphore_signal(barrier, inc=1, device_id={AXES[dim]: me[dim] + shift}, device_id_type=MESH)

    pl.semaphore_wait(barrier, greeted)


def each_side(me, has, dim, act, copy_of, also=None):
    incoming = act == "recv"
    for side, shift in enumerate((-1, 1)):
        there = has[dim][1 - side if incoming else side]
        if also is not None:
            there = jnp.logical_and(there, also)

        @pl.when(there)
        def _():
            copy = copy_of(side, me[dim] - shift if incoming else me[dim] + shift)
            if incoming:
                copy.wait_recv()
            elif act == "send":
                copy.wait_send()
            else:
                copy.start()


def main_kernel(
    counts,
    bounds,
    start_ref,
    earlier_ref,
    speed_ref,
    end_ref,
    edge_ref,
    pace_ref,
    even,
    odd,
    speed,
    load_sem,
    lat_send,
    lat_recv,
    side_send,
    side_recv,
):
    rows, columns, depth, lanes = start_ref.shape
    fields = (even, odd)
    inside = pl.ds(PAD, depth)
    me, has = neighbours(counts)
    parts = [(first, after - first) for first, after in zip(bounds, bounds[1:])]
    split, final = bounds[1], len(parts) - 1
    early_first, early_width = parts[final]

    edges = (0, rows - 1)
    early = [
        pltpu.make_async_copy(
            start_ref.at[plane, pl.ds(early_first, early_width)],
            even.at[plane + 1, pl.ds(1 + early_first, early_width), inside],
            load_sem.at[place],
        )
        for place, plane in enumerate(edges)
    ]
    loads = [
        pltpu.make_async_copy(earlier_ref, odd.at[pl.ds(1, rows), pl.ds(1, columns), inside], load_sem.at[2]),
        pltpu.make_async_copy(speed_ref, speed, load_sem.at[3]),
    ] + [
        pltpu.make_async_copy(
            start_ref.at[plane, pl.ds(0, early_first)],
            even.at[plane + 1, pl.ds(1, early_first), inside],
            load_sem.at[4 + place],
        )
        for place, plane in enumerate(edges)
    ]
    loads += [
        pltpu.make_async_copy(
            speed_ref.at[plane, pl.ds(split, columns - split)], pace_ref.at[place], load_sem.at[6 + place]
        )
        for place, plane in enumerate(edges)
    ]
    if rows > 2:
        loads.append(
            pltpu.make_async_copy(
                start_ref.at[pl.ds(1, rows - 2)],
                even.at[pl.ds(2, rows - 2), pl.ds(1, columns), inside],
                load_sem.at[8],
            )
        )
    for load in early:
        load.start()

    greet(me, has, (0, 1, 2))

    def lat_each(step, part, act, held=False):
        field = fields[step % 2]
        first, width = parts[part]

        def copy_of(side, target):
            if step == 0 and not held:
                source = start_ref.at[(0, rows - 1)[side], pl.ds(first, width)]
            else:
                source = field.at[(1, rows)[side], pl.ds(first + 1, width), inside]
            return pltpu.make_async_remote_copy(
                src_ref=source,
                dst_ref=field.at[(rows + 1, 0)[side], pl.ds(first + 1, width), inside],
                send_sem=lat_send.at[side, part],
                recv_sem=lat_recv.at[step % 2, side, part],
                device_id={"lat": target},
                device_id_type=MESH,
            )

        also = late() if step == STEPS - 1 and part > 0 else None
        each_side(me, has, 0, act, copy_of, also)

    def side_each(step, act):
        field = fields[step % 2]
        for dim in (1, 2):

            def copy_of(side, target):
                if dim == 1:
                    if step == 0:
                        source = start_ref.at[:, (0, columns - 1)[side]]
                    else:
                        source = field.at[pl.ds(1, rows), (1, columns)[side], inside]
                    dest = field.at[pl.ds(1, rows), (columns + 1, 0)[side], inside]
                else:
                    if step == 0:
                        source = start_ref.at[:, :, pl.ds((0, depth - PAD)[side], PAD)]
                    else:
                        source = field.at[pl.ds(1, rows), pl.ds(1, columns), pl.ds((PAD, depth)[side], PAD)]
                    dest = field.at[pl.ds(1, rows), pl.ds(1, columns), pl.ds((PAD + depth, 0)[side], PAD)]
                return pltpu.make_async_remote_copy(
                    src_ref=source,
                    dst_ref=dest,
                    send_sem=side_send.at[dim - 1, side],
                    recv_sem=side_recv.at[step % 2, dim - 1, side],
                    device_id={AXES[dim]: target},
                    device_id_type=MESH,
                )

            each_side(me, has, dim, act, copy_of)

    for load in early:
        load.wait()
    lat_each(0, final, "start", held=True)
    for part in range(final):
        lat_each(0, part, "start")
    side_each(0, "start")
    for load in loads:
        load.start()

    for side in (0, 1):

        @pl.when(jnp.logical_not(has[0][side]))
        def _():
            @pl.loop(1, columns + 1)
            def _(x):
                for field in fields:
                    field[(0, rows + 1)[side], x, inside] = jnp.zeros((depth, lanes), jnp.float32)

        @pl.when(jnp.logical_not(has[1][side]))
        def _():
            for field in fields:
                for y in range(1, rows + 1):
                    field[y, (0, columns + 1)[side], inside] = jnp.zeros((depth, lanes), jnp.float32)

        @pl.when(jnp.logical_not(has[2][side]))
        def _():
            @pl.loop(1, columns + 1)
            def _(x):
                for field in fields:
                    for y in range(1, rows + 1):
                        field[y, x, pl.ds((0, PAD + depth)[side], PAD)] = jnp.zeros((PAD, lanes), jnp.float32)

    for load in loads:
        load.wait()

    def advance(step, y, x, low=True, high=True):
        now, other = fields[step % 2], fields[(step + 1) % 2]
        middle = now[y, x, inside]
        spread = now[y, x - 1, inside] + now[y, x + 1, inside]
        if low:
            spread += now[y - 1, x, inside]
        if high:
            spread += now[y + 1, x, inside]
        spread += now[y, x, pl.ds(PAD - 1, depth)] + now[y, x, pl.ds(PAD + 1, depth)] - 6.0 * middle
        return 2.0 * middle - other[y, x, inside] + speed[y - 1, x - 1] * spread

    for step in range(STEPS - 1):
        other = fields[(step + 1) % 2]
        side_each(step, "recv")
        side_each(step, "send")
        for part, (first, width) in enumerate(parts):
            lat_each(step, part, "recv")
            lat_each(step, part, "send", held=part == final)
            keep = step == STEPS - 2 and part > 0

            @pl.loop(first + 1, first + width + 1)
            def _(x):
                for place, y in enumerate((1, rows)):
                    later = advance(step, y, x)
                    other[y, x, inside] = later
                    if keep:
                        edge_ref[place, x - 1 - split] = later

            lat_each(step + 1, part, "start") if part == 0 or step < STEPS - 2 else None
            if step == STEPS - 2 and 0 < part < final:
                lat_each(step + 1, part, "start")

            @pl.loop(first + 1, first + width + 1)
            def _(x):
                for y in range(2, rows):
                    other[y, x, inside] = advance(step, y, x)

        side_each(step + 1, "start")

    step = STEPS - 1
    now = fields[step % 2]
    side_each(step, "recv")

    @pl.loop(1, columns + 1)
    def _(x):
        for y in range(1, rows + 1):
            end_ref[y - 1, x - 1] = advance(step, y, x, low=y > 1, high=y < rows)

    side_each(step, "send")
    for part, (first, width) in enumerate(parts[:-1]):
        lat_each(step, part, "recv")

        def finish():
            @pl.loop(first, first + width)
            def _(x):
                for row, halo in ((0, 0), (rows - 1, rows + 1)):
                    end_ref[row, x] = end_ref[row, x] + speed[row, x] * now[halo, x + 1, inside]

        finish() if part == 0 else pl.when(late())(finish)
        lat_each(step, part, "send")


def tail_kernel(counts, bounds, end_ref, edge_ref, pace_ref, token_ref, last_ref, halo, send, recv):
    rows = end_ref.shape[0]
    split, columns = bounds[1], bounds[-1]
    me, has = neighbours(counts)
    greet(me, has, (0,))
    parts = list(enumerate(zip(bounds[1:], bounds[2:])))

    def lat_each(part, first, after, act):
        span = pl.ds(first - split, after - first)

        def copy_of(side, target):
            return pltpu.make_async_remote_copy(
                src_ref=edge_ref.at[side, span],
                dst_ref=halo.at[1 - side, span],
                send_sem=send.at[side, part],
                recv_sem=recv.at[side, part],
                device_id={"lat": target},
                device_id_type=MESH,
            )

        each_side(me, has, 0, act, copy_of, None if part == len(parts) - 1 else jnp.logical_not(late()))

    for part, (first, after) in parts:
        lat_each(part, first, after, "start")
    for part, (first, after) in parts:
        lat_each(part, first, after, "recv")

        def finish():
            for place, row in enumerate((0, rows - 1)):

                @pl.when(has[0][place])
                def _():
                    @pl.loop(first, after)
                    def _(x):
                        last_ref[place, x - split] = end_ref[row, x] + pace_ref[place, x - split] * halo[place, x - split]

                @pl.when(jnp.logical_not(has[0][place]))
                def _():
                    @pl.loop(first, after)
                    def _(x):
                        last_ref[place, x - split] = end_ref[row, x]

        finish() if part == len(parts) - 1 else pl.when(jnp.logical_not(late()))(finish)
    for part, (first, after) in parts:
        lat_each(part, first, after, "send")


def run(copies, there=None):
    def go():
        for copy in copies:
            copy.start()
        for copy in copies:
            copy.wait()

    go() if there is None else pl.when(there)(go)


def write_kernel(bounds, end_ref, out_ref, token_ref, sem):
    token_ref[...] = jnp.zeros_like(token_ref)
    rows, columns = out_ref.shape[:2]
    split, after = bounds[1], bounds[2]
    pieces = [(0, pl.ds(0, split)), (rows - 1, pl.ds(0, split))] + [(row, pl.ds(0, columns)) for row in range(1, rows - 1)]
    more = [(0, pl.ds(split, after - split)), (rows - 1, pl.ds(split, after - split))]
    copies = [
        pltpu.make_async_copy(end_ref.at[row, span], out_ref.at[row, span], sem.at[place])
        for place, (row, span) in enumerate(pieces + more)
    ]
    lagging = copies[len(pieces) :]

    @pl.when(late())
    def _():
        for copy in lagging:
            copy.start()

    run(copies[: len(pieces)])

    @pl.when(late())
    def _():
        for copy in lagging:
            copy.wait()


def patch_kernel(bounds, whole_ref, last_ref, out_ref, sem):
    rows, columns = out_ref.shape[:2]
    split = bounds[1]
    for first, there in ((split, jnp.logical_not(late())), (bounds[2], late())):
        run(
            [
                pltpu.make_async_copy(
                    last_ref.at[place, pl.ds(first - split, columns - first)],
                    out_ref.at[row, pl.ds(first, columns - first)],
                    sem.at[place],
                )
                for place, row in enumerate((0, rows - 1))
            ],
            there,
        )


def solution(mesh):
    counts = tuple(mesh.shape[axis] for axis in AXES)
    vmem, hbm = pl.BlockSpec(memory_space=pltpu.VMEM), pl.BlockSpec(memory_space=pltpu.HBM)
    dma = pltpu.SemaphoreType.DMA

    def shards(pressure, earlier, speed_square):
        rows, columns, depth, lanes = pressure.shape
        bounds = (0,) + tuple(columns - columns * tail // 64 for tail in TAILS) + (columns,)
        parts = len(bounds) - 1
        edge = (2, columns - bounds[1], depth, lanes)
        field = pltpu.VMEM((rows + 2, columns + 2, depth + 2 * PAD, lanes), jnp.float32)
        end, edges, paces = pl.pallas_call(
            functools.partial(main_kernel, counts, bounds),
            out_shape=(pltpu.VMEM(pressure.shape, jnp.float32), pltpu.VMEM(edge, jnp.float32), pltpu.VMEM(edge, jnp.float32)),
            in_specs=[hbm] * 3,
            out_specs=(vmem,) * 3,
            scratch_shapes=[
                field,
                field,
                pltpu.VMEM(pressure.shape, jnp.float32),
                dma((9,)),
                dma((2, parts)),
                dma((2, 2, parts)),
                dma((2, 2)),
                dma((2, 2, 2)),
            ],
            compiler_params=pltpu.CompilerParams(
                collective_id=0, has_side_effects=True, vmem_limit_bytes=44 * 2**20
            ),
        )(pressure, earlier, speed_square)
        out, token = pl.pallas_call(
            functools.partial(write_kernel, bounds),
            out_shape=(pltpu.HBM(pressure.shape, jnp.float32), pltpu.VMEM((8, 128), jnp.float32)),
            in_specs=[vmem],
            out_specs=(hbm, vmem),
            scratch_shapes=[dma((rows + 2,))],
            compiler_params=pltpu.CompilerParams(vmem_limit_bytes=2**20),
        )(end)
        last = pl.pallas_call(
            functools.partial(tail_kernel, counts, bounds),
            out_shape=pltpu.VMEM(edge, jnp.float32),
            in_specs=[vmem] * 4,
            out_specs=vmem,
            scratch_shapes=[
                pltpu.VMEM(edge, jnp.float32),
                dma((2, parts - 1)),
                dma((2, parts - 1)),
            ],
            compiler_params=pltpu.CompilerParams(
                collective_id=1, has_side_effects=True, vmem_limit_bytes=4 * 2**20
            ),
        )(end, edges, paces, token)
        return pl.pallas_call(
            functools.partial(patch_kernel, bounds),
            out_shape=pltpu.HBM(pressure.shape, jnp.float32),
            in_specs=[hbm, vmem],
            out_specs=hbm,
            input_output_aliases={0: 0},
            scratch_shapes=[dma((2,))],
            compiler_params=pltpu.CompilerParams(vmem_limit_bytes=2**20),
        )(out, last)

    spec = P("lat", "lon", "lev", None)
    return jax.shard_map(shards, mesh=mesh, in_specs=(spec, spec, spec), out_specs=spec, check_vma=False)
```

```python
import functools

import jax
import jax.numpy as jnp
from jax import lax
from jax.experimental import pallas as pl
from jax.experimental.pallas import tpu as pltpu
from jax.sharding import PartitionSpec as P

STEPS = 4
TAILS = (24, 8)
PAD = 8
AXES = ("lat", "lon", "lev")
MESH = pl.DeviceIdType.MESH


def late():
    return lax.axis_index("lev") % 2 == 0


def neighbours(counts):
    me = [lax.axis_index(axis) for axis in AXES]
    return me, [(place > 0, place < count - 1) for place, count in zip(me, counts)]


def greet(me, has, dims):
    barrier = pltpu.get_barrier_semaphore()
    greeted = jnp.int32(0)
    for dim in dims:
        for side, shift in enumerate((-1, 1)):
            greeted = greeted + has[dim][side].astype(jnp.int32)

            @pl.when(has[dim][side])
            def _():
                pl.semaphore_signal(barrier, inc=1, device_id={AXES[dim]: me[dim] + shift}, device_id_type=MESH)

    pl.semaphore_wait(barrier, greeted)


def each_side(me, has, dim, act, copy_of, also=None, sides=(0, 1)):
    incoming = act == "recv"
    for side in sides:
        shift = (-1, 1)[side]
        there = has[dim][1 - side if incoming else side]
        if also is not None:
            there = jnp.logical_and(there, also)

        @pl.when(there)
        def _():
            copy = copy_of(side, me[dim] - shift if incoming else me[dim] + shift)
            if incoming:
                copy.wait_recv()
            elif act == "send":
                copy.wait_send()
            else:
                copy.start()


def main_kernel(
    counts,
    bounds,
    start_ref,
    earlier_ref,
    speed_ref,
    end_ref,
    edge_ref,
    pace_ref,
    even,
    odd,
    speed,
    load_sem,
    lat_send,
    lat_recv,
    side_send,
    side_recv,
    reply_sem,
    level_sem,
    beside_sem,
):
    rows, columns, depth, lanes = start_ref.shape
    fields = (even, odd)
    inside = pl.ds(PAD, depth)
    me, has = neighbours(counts)
    parts = [(first, after - first) for first, after in zip(bounds, bounds[1:])]
    split, final = bounds[1], len(parts) - 1
    early_first, early_width = parts[final]

    edges = (0, rows - 1)
    early = [
        pltpu.make_async_copy(
            start_ref.at[plane, pl.ds(early_first, early_width)],
            even.at[plane + 1, pl.ds(1 + early_first, early_width), inside],
            load_sem.at[place],
        )
        for place, plane in enumerate(edges)
    ]
    loads = [
        pltpu.make_async_copy(earlier_ref, odd.at[pl.ds(1, rows), pl.ds(1, columns), inside], load_sem.at[2]),
        pltpu.make_async_copy(speed_ref, speed, load_sem.at[3]),
    ] + [
        pltpu.make_async_copy(
            start_ref.at[plane, pl.ds(0, early_first)],
            even.at[plane + 1, pl.ds(1, early_first), inside],
            load_sem.at[4 + place],
        )
        for place, plane in enumerate(edges)
    ]
    loads += [
        pltpu.make_async_copy(
            speed_ref.at[plane, pl.ds(split, columns - split)], pace_ref.at[place], load_sem.at[6 + place]
        )
        for place, plane in enumerate(edges)
    ]
    if rows > 2:
        loads.append(
            pltpu.make_async_copy(
                start_ref.at[pl.ds(1, rows - 2)],
                even.at[pl.ds(2, rows - 2), pl.ds(1, columns), inside],
                load_sem.at[8],
            )
        )
    for load in early:
        load.start()

    low, high = has[0]
    bottom = jnp.logical_not(low)
    barrier = pltpu.get_barrier_semaphore()
    beside = sum(there.astype(jnp.int32) for dim in (1, 2) for there in has[dim])

    def tell_beside(sem):
        for dim in (1, 2):
            for side, shift in enumerate((-1, 1)):

                @pl.when(has[dim][side])
                def _():
                    pl.semaphore_signal(sem, inc=1, device_id={AXES[dim]: me[dim] + shift}, device_id_type=MESH)

    @pl.when(high)
    def _():
        pl.semaphore_signal(barrier, inc=1, device_id={"lat": me[0] + 1}, device_id_type=MESH)

    @pl.when(bottom)
    def _():
        tell_beside(barrier)

    def lat_each(step, part, act, held=False, sides=(0, 1)):
        field = fields[step % 2]
        first, width = parts[part]

        def copy_of(side, target):
            if step == 0 and not held:
                source = start_ref.at[(0, rows - 1)[side], pl.ds(first, width)]
            else:
                source = field.at[(1, rows)[side], pl.ds(first + 1, width), inside]
            return pltpu.make_async_remote_copy(
                src_ref=source,
                dst_ref=field.at[(rows + 1, 0)[side], pl.ds(first + 1, width), inside],
                send_sem=lat_send.at[side, part],
                recv_sem=lat_recv.at[step % 2, side, part],
                device_id={"lat": target},
                device_id_type=MESH,
            )

        also = late() if step == STEPS - 1 and part > 0 else None
        each_side(me, has, 0, act, copy_of, also, sides)

    def side_each(step, act):
        field = fields[step % 2]
        for dim in (1, 2):

            def copy_of(side, target):
                if dim == 1:
                    if step == 0:
                        source = start_ref.at[:, (0, columns - 1)[side]]
                    else:
                        source = field.at[pl.ds(1, rows), (1, columns)[side], inside]
                    dest = field.at[pl.ds(1, rows), (columns + 1, 0)[side], inside]
                else:
                    if step == 0:
                        source = start_ref.at[:, :, pl.ds((0, depth - PAD)[side], PAD)]
                    else:
                        source = field.at[pl.ds(1, rows), pl.ds(1, columns), pl.ds((PAD, depth)[side], PAD)]
                    dest = field.at[pl.ds(1, rows), pl.ds(1, columns), pl.ds((PAD + depth, 0)[side], PAD)]
                return pltpu.make_async_remote_copy(
                    src_ref=source,
                    dst_ref=dest,
                    send_sem=side_send.at[dim - 1, side],
                    recv_sem=side_recv.at[step % 2, dim - 1, side],
                    device_id={AXES[dim]: target},
                    device_id_type=MESH,
                )

            each_side(me, has, dim, act, copy_of)

    for load in early:
        load.wait()

    def lat_first(side):
        lat_each(0, final, "start", held=True, sides=(side,))
        for part in range(final):
            lat_each(0, part, "start", sides=(side,))

    @pl.when(low)
    def _():
        pl.semaphore_wait(barrier, 1)
        pl.semaphore_signal(reply_sem, inc=1, device_id={"lat": me[0] - 1}, device_id_type=MESH)

    lat_first(0)

    @pl.when(high)
    def _():
        pl.semaphore_wait(reply_sem, 1)

    lat_first(1)
    for load in loads:
        load.start()

    @pl.when(bottom)
    def _():
        pl.semaphore_wait(barrier, beside)

    @pl.when(low)
    def _():
        pl.semaphore_wait(level_sem, 1)

    @pl.when(high)
    def _():
        tell_beside(beside_sem)
        pl.semaphore_wait(beside_sem, beside)
        pl.semaphore_signal(level_sem, inc=1, device_id={"lat": me[0] + 1}, device_id_type=MESH)

    side_each(0, "start")

    for side in (0, 1):

        @pl.when(jnp.logical_not(has[0][side]))
        def _():
            @pl.loop(1, columns + 1)
            def _(x):
                for field in fields:
                    field[(0, rows + 1)[side], x, inside] = jnp.zeros((depth, lanes), jnp.float32)

        @pl.when(jnp.logical_not(has[1][side]))
        def _():
            for field in fields:
                for y in range(1, rows + 1):
                    field[y, (0, columns + 1)[side], inside] = jnp.zeros((depth, lanes), jnp.float32)

        @pl.when(jnp.logical_not(has[2][side]))
        def _():
            @pl.loop(1, columns + 1)
            def _(x):
                for field in fields:
                    for y in range(1, rows + 1):
                        field[y, x, pl.ds((0, PAD + depth)[side], PAD)] = jnp.zeros((PAD, lanes), jnp.float32)

    for load in loads:
        load.wait()

    def advance(step, y, x, low=True, high=True):
        now, other = fields[step % 2], fields[(step + 1) % 2]
        middle = now[y, x, inside]
        spread = now[y, x - 1, inside] + now[y, x + 1, inside]
        if low:
            spread += now[y - 1, x, inside]
        if high:
            spread += now[y + 1, x, inside]
        spread += now[y, x, pl.ds(PAD - 1, depth)] + now[y, x, pl.ds(PAD + 1, depth)] - 6.0 * middle
        return 2.0 * middle - other[y, x, inside] + speed[y - 1, x - 1] * spread

    for step in range(STEPS - 1):
        other = fields[(step + 1) % 2]
        side_each(step, "recv")
        side_each(step, "send")
        for part, (first, width) in enumerate(parts):
            lat_each(step, part, "recv")
            lat_each(step, part, "send", held=part == final)
            keep = step == STEPS - 2 and part > 0

            @pl.loop(first + 1, first + width + 1)
            def _(x):
                for place, y in enumerate((1, rows)):
                    later = advance(step, y, x)
                    other[y, x, inside] = later
                    if keep:
                        edge_ref[place, x - 1 - split] = later

            lat_each(step + 1, part, "start")

            @pl.loop(first + 1, first + width + 1)
            def _(x):
                for y in range(2, rows):
                    other[y, x, inside] = advance(step, y, x)

        side_each(step + 1, "start")

    step = STEPS - 1
    now = fields[step % 2]
    side_each(step, "recv")

    @pl.loop(1, columns + 1)
    def _(x):
        for y in range(1, rows + 1):
            end_ref[y - 1, x - 1] = advance(step, y, x, low=y > 1, high=y < rows)

    side_each(step, "send")
    for part, (first, width) in enumerate(parts):
        lat_each(step, part, "recv")

        def finish():
            @pl.loop(first, first + width)
            def _(x):
                for row, halo in ((0, 0), (rows - 1, rows + 1)):
                    end_ref[row, x] = end_ref[row, x] + speed[row, x] * now[halo, x + 1, inside]

        finish() if part == 0 else pl.when(late())(finish)
        lat_each(step, part, "send")


def tail_kernel(counts, bounds, end_ref, edge_ref, pace_ref, token_ref, last_ref, halo, send, recv):
    rows = end_ref.shape[0]
    split, columns = bounds[1], bounds[-1]
    me, has = neighbours(counts)
    mine = jnp.logical_not(late())

    @pl.when(mine)
    def _():
        greet(me, has, (0,))

    parts = list(enumerate(zip(bounds[1:], bounds[2:])))

    def lat_each(part, first, after, act):
        span = pl.ds(first - split, after - first)

        def copy_of(side, target):
            return pltpu.make_async_remote_copy(
                src_ref=edge_ref.at[side, span],
                dst_ref=halo.at[1 - side, span],
                send_sem=send.at[side, part],
                recv_sem=recv.at[side, part],
                device_id={"lat": target},
                device_id_type=MESH,
            )

        each_side(me, has, 0, act, copy_of, mine)

    for part, (first, after) in parts:
        lat_each(part, first, after, "start")
    for part, (first, after) in parts:
        lat_each(part, first, after, "recv")

        def finish():
            for place, row in enumerate((0, rows - 1)):

                @pl.when(has[0][place])
                def _():
                    @pl.loop(first, after)
                    def _(x):
                        last_ref[place, x - split] = end_ref[row, x] + pace_ref[place, x - split] * halo[place, x - split]

                @pl.when(jnp.logical_not(has[0][place]))
                def _():
                    @pl.loop(first, after)
                    def _(x):
                        last_ref[place, x - split] = end_ref[row, x]

        pl.when(mine)(finish)
    for part, (first, after) in parts:
        lat_each(part, first, after, "send")


def run(copies, there=None):
    def go():
        for copy in copies:
            copy.start()
        for copy in copies:
            copy.wait()

    go() if there is None else pl.when(there)(go)


def write_kernel(bounds, end_ref, out_ref, token_ref, sem):
    token_ref[...] = jnp.zeros_like(token_ref)
    rows, columns = out_ref.shape[:2]
    split = bounds[1]
    pieces = [(0, pl.ds(0, split)), (rows - 1, pl.ds(0, split))] + [(row, pl.ds(0, columns)) for row in range(1, rows - 1)]
    more = [(0, pl.ds(split, columns - split)), (rows - 1, pl.ds(split, columns - split))]
    copies = [
        pltpu.make_async_copy(end_ref.at[row, span], out_ref.at[row, span], sem.at[place])
        for place, (row, span) in enumerate(pieces + more)
    ]
    lagging = copies[len(pieces) :]

    @pl.when(late())
    def _():
        for copy in lagging:
            copy.start()

    run(copies[: len(pieces)])

    @pl.when(late())
    def _():
        for copy in lagging:
            copy.wait()


def patch_kernel(bounds, whole_ref, last_ref, out_ref, sem):
    rows, columns = out_ref.shape[:2]
    span = pl.ds(bounds[1], columns - bounds[1])
    run(
        [
            pltpu.make_async_copy(last_ref.at[place], out_ref.at[row, span], sem.at[place])
            for place, row in enumerate((0, rows - 1))
        ],
        jnp.logical_not(late()),
    )


def solution(mesh):
    counts = tuple(mesh.shape[axis] for axis in AXES)
    vmem, hbm = pl.BlockSpec(memory_space=pltpu.VMEM), pl.BlockSpec(memory_space=pltpu.HBM)
    dma = pltpu.SemaphoreType.DMA

    def shards(pressure, earlier, speed_square):
        rows, columns, depth, lanes = pressure.shape
        bounds = (0,) + tuple(columns - columns * tail // 64 for tail in TAILS) + (columns,)
        parts = len(bounds) - 1
        edge = (2, columns - bounds[1], depth, lanes)
        field = pltpu.VMEM((rows + 2, columns + 2, depth + 2 * PAD, lanes), jnp.float32)
        end, edges, paces = pl.pallas_call(
            functools.partial(main_kernel, counts, bounds),
            out_shape=(pltpu.VMEM(pressure.shape, jnp.float32), pltpu.VMEM(edge, jnp.float32), pltpu.VMEM(edge, jnp.float32)),
            in_specs=[hbm] * 3,
            out_specs=(vmem,) * 3,
            scratch_shapes=[
                field,
                field,
                pltpu.VMEM(pressure.shape, jnp.float32),
                dma((9,)),
                dma((2, parts)),
                dma((2, 2, parts)),
                dma((2, 2)),
                dma((2, 2, 2)),
            ]
            + [pltpu.SemaphoreType.REGULAR] * 3,
            compiler_params=pltpu.CompilerParams(
                collective_id=0, has_side_effects=True, vmem_limit_bytes=44 * 2**20
            ),
        )(pressure, earlier, speed_square)
        out, token = pl.pallas_call(
            functools.partial(write_kernel, bounds),
            out_shape=(pltpu.HBM(pressure.shape, jnp.float32), pltpu.VMEM((8, 128), jnp.float32)),
            in_specs=[vmem],
            out_specs=(hbm, vmem),
            scratch_shapes=[dma((rows + 2,))],
            compiler_params=pltpu.CompilerParams(vmem_limit_bytes=2**20),
        )(end)
        last = pl.pallas_call(
            functools.partial(tail_kernel, counts, bounds),
            out_shape=pltpu.VMEM(edge, jnp.float32),
            in_specs=[vmem] * 4,
            out_specs=vmem,
            scratch_shapes=[
                pltpu.VMEM(edge, jnp.float32),
                dma((2, parts - 1)),
                dma((2, parts - 1)),
            ],
            compiler_params=pltpu.CompilerParams(
                collective_id=1, has_side_effects=True, vmem_limit_bytes=4 * 2**20
            ),
        )(end, edges, paces, token)
        return pl.pallas_call(
            functools.partial(patch_kernel, bounds),
            out_shape=pltpu.HBM(pressure.shape, jnp.float32),
            in_specs=[hbm, vmem],
            out_specs=hbm,
            input_output_aliases={0: 0},
            scratch_shapes=[dma((2,))],
            compiler_params=pltpu.CompilerParams(vmem_limit_bytes=2**20),
        )(out, last)

    spec = P("lat", "lon", "lev", None)
    return jax.shard_map(shards, mesh=mesh, in_specs=(spec, spec, spec), out_specs=spec, check_vma=False)
```

```python
import functools

import jax
import jax.numpy as jnp
from jax import lax
from jax.experimental import pallas as pl
from jax.experimental.pallas import tpu as pltpu
from jax.sharding import PartitionSpec as P

STEPS = 4
TAIL = 20
EARLY = 4
END = 2
PAD = 8
AXES = ("lat", "lon", "lev")
MESH = pl.DeviceIdType.MESH


def late():
    return lax.axis_index("lev") % 2 == 0


def neighbours(counts):
    me = [lax.axis_index(axis) for axis in AXES]
    return me, [(place > 0, place < count - 1) for place, count in zip(me, counts)]


def greet(me, has, dims):
    barrier = pltpu.get_barrier_semaphore()
    greeted = jnp.int32(0)
    for dim in dims:
        for side, shift in enumerate((-1, 1)):
            greeted = greeted + has[dim][side].astype(jnp.int32)

            @pl.when(has[dim][side])
            def _():
                pl.semaphore_signal(barrier, inc=1, device_id={AXES[dim]: me[dim] + shift}, device_id_type=MESH)

    pl.semaphore_wait(barrier, greeted)


def each_side(me, has, dim, act, copy_of, also=None, sides=(0, 1)):
    incoming = act == "recv"
    for side in sides:
        shift = (-1, 1)[side]
        there = has[dim][1 - side if incoming else side]
        if also is not None:
            there = jnp.logical_and(there, also)

        @pl.when(there)
        def _():
            copy = copy_of(side, me[dim] - shift if incoming else me[dim] + shift)
            if incoming:
                copy.wait_recv()
            elif act == "send":
                copy.wait_send()
            else:
                copy.start()


def main_kernel(
    counts,
    bounds,
    early_first,
    start_ref,
    earlier_ref,
    speed_ref,
    end_ref,
    edge_ref,
    pace_ref,
    even,
    odd,
    speed,
    load_sem,
    lat_send,
    lat_recv,
    side_send,
    side_recv,
    reply_sem,
    level_sem,
    beside_sem,
):
    rows, columns, depth, lanes = start_ref.shape
    fields = (even, odd)
    inside = pl.ds(PAD, depth)
    me, has = neighbours(counts)
    parts = [(first, after - first) for first, after in zip(bounds, bounds[1:])]
    split = bounds[1]

    early = [
        pltpu.make_async_copy(
            start_ref.at[plane, pl.ds(early_first, columns - early_first)],
            even.at[plane + 1, pl.ds(1 + early_first, columns - early_first), inside],
            load_sem.at[place],
        )
        for place, plane in enumerate((0, rows - 1))
    ]
    starts = [
        pltpu.make_async_copy(
            start_ref.at[:, pl.ds(0, early_first)],
            even.at[pl.ds(1, rows), pl.ds(1, early_first), inside],
            load_sem.at[2],
        )
    ]
    if rows > 2:
        starts.append(
            pltpu.make_async_copy(
                start_ref.at[pl.ds(1, rows - 2), pl.ds(early_first, columns - early_first)],
                even.at[pl.ds(2, rows - 2), pl.ds(1 + early_first, columns - early_first), inside],
                load_sem.at[3],
            )
        )
    loads = [
        pltpu.make_async_copy(earlier_ref, odd.at[pl.ds(1, rows), pl.ds(1, columns), inside], load_sem.at[4]),
        pltpu.make_async_copy(speed_ref, speed, load_sem.at[5]),
    ]
    behind = late()
    ahead = jnp.logical_not(behind)

    for load in early:
        load.start()

    @pl.when(behind)
    def _():
        for load in starts:
            load.start()

    low, high = has[0]
    bottom = jnp.logical_not(low)
    barrier = pltpu.get_barrier_semaphore()
    beside = sum(there.astype(jnp.int32) for dim in (1, 2) for there in has[dim])

    def tell_beside(sem):
        for dim in (1, 2):
            for side, shift in enumerate((-1, 1)):

                @pl.when(has[dim][side])
                def _():
                    pl.semaphore_signal(sem, inc=1, device_id={AXES[dim]: me[dim] + shift}, device_id_type=MESH)

    @pl.when(high)
    def _():
        pl.semaphore_signal(barrier, inc=1, device_id={"lat": me[0] + 1}, device_id_type=MESH)

    @pl.when(bottom)
    def _():
        tell_beside(barrier)

    @pl.when(low)
    def _():
        pl.semaphore_wait(barrier, 1)
        pl.semaphore_signal(reply_sem, inc=1, device_id={"lat": me[0] - 1}, device_id_type=MESH)

    def lat_piece(step, part, act, first, width, also=None, sides=(0, 1), held=True):
        field = fields[step % 2]

        def copy_of(side, target):
            if held:
                source = field.at[(1, rows)[side], pl.ds(first + 1, width), inside]
            else:
                source = start_ref.at[(0, rows - 1)[side], pl.ds(first, width)]
            return pltpu.make_async_remote_copy(
                src_ref=source,
                dst_ref=field.at[(rows + 1, 0)[side], pl.ds(first + 1, width), inside],
                send_sem=lat_send.at[side, part],
                recv_sem=lat_recv.at[step % 2, side, part],
                device_id={"lat": target},
                device_id_type=MESH,
            )

        each_side(me, has, 0, act, copy_of, also, sides)

    def lat_each(step, part, act):
        lat_piece(step, part, act, *parts[part], behind if step == STEPS - 1 and part > 0 else None)

    def lat_first(side):
        lat_piece(0, 1, "start", early_first, columns - early_first, ahead, (side,))
        lat_piece(0, 0, "start", 0, split, ahead, (side,), held=False)
        lat_piece(0, 1, "start", split, early_first - split, ahead, (side,), held=False)
        for part, piece in enumerate(parts):
            lat_piece(0, part, "start", *piece, behind, (side,))

    def side_each(step, act):
        field = fields[step % 2]
        for dim in (1, 2):

            def copy_of(side, target):
                if dim == 1:
                    if step == 0:
                        source = start_ref.at[:, (0, columns - 1)[side]]
                    else:
                        source = field.at[pl.ds(1, rows), (1, columns)[side], inside]
                    dest = field.at[pl.ds(1, rows), (columns + 1, 0)[side], inside]
                else:
                    if step == 0:
                        source = start_ref.at[:, :, pl.ds((0, depth - PAD)[side], PAD)]
                    else:
                        source = field.at[pl.ds(1, rows), pl.ds(1, columns), pl.ds((PAD, depth)[side], PAD)]
                    dest = field.at[pl.ds(1, rows), pl.ds(1, columns), pl.ds((PAD + depth, 0)[side], PAD)]
                return pltpu.make_async_remote_copy(
                    src_ref=source,
                    dst_ref=dest,
                    send_sem=side_send.at[dim - 1, side],
                    recv_sem=side_recv.at[step % 2, dim - 1, side],
                    device_id={AXES[dim]: target},
                    device_id_type=MESH,
                )

            each_side(me, has, dim, act, copy_of)

    for load in early:
        load.wait()

    @pl.when(behind)
    def _():
        for load in starts:
            load.wait()

    lat_first(0)

    @pl.when(high)
    def _():
        pl.semaphore_wait(reply_sem, 1)

    lat_first(1)

    @pl.when(ahead)
    def _():
        for load in starts:
            load.start()

    for load in loads:
        load.start()

    @pl.when(bottom)
    def _():
        pl.semaphore_wait(barrier, beside)

    @pl.when(low)
    def _():
        pl.semaphore_wait(level_sem, 1)

    @pl.when(high)
    def _():
        tell_beside(beside_sem)
        pl.semaphore_wait(beside_sem, beside)
        pl.semaphore_signal(level_sem, inc=1, device_id={"lat": me[0] + 1}, device_id_type=MESH)

    side_each(0, "start")

    for side in (0, 1):

        @pl.when(jnp.logical_not(has[0][side]))
        def _():
            @pl.loop(1, columns + 1)
            def _(x):
                for field in fields:
                    field[(0, rows + 1)[side], x, inside] = jnp.zeros((depth, lanes), jnp.float32)

        @pl.when(jnp.logical_not(has[1][side]))
        def _():
            for field in fields:
                for y in range(1, rows + 1):
                    field[y, (0, columns + 1)[side], inside] = jnp.zeros((depth, lanes), jnp.float32)

        @pl.when(jnp.logical_not(has[2][side]))
        def _():
            @pl.loop(1, columns + 1)
            def _(x):
                for field in fields:
                    for y in range(1, rows + 1):
                        field[y, x, pl.ds((0, PAD + depth)[side], PAD)] = jnp.zeros((PAD, lanes), jnp.float32)

    @pl.when(ahead)
    def _():
        for load in starts:
            load.wait()

    for load in loads:
        load.wait()

    def advance(step, y, x, low=True, high=True):
        now, other = fields[step % 2], fields[(step + 1) % 2]
        middle = now[y, x, inside]
        spread = now[y, x - 1, inside] + now[y, x + 1, inside]
        if low:
            spread += now[y - 1, x, inside]
        if high:
            spread += now[y + 1, x, inside]
        spread += now[y, x, pl.ds(PAD - 1, depth)] + now[y, x, pl.ds(PAD + 1, depth)] - 6.0 * middle
        return 2.0 * middle - other[y, x, inside] + speed[y - 1, x - 1] * spread

    for step in range(STEPS - 1):
        other = fields[(step + 1) % 2]
        side_each(step, "recv")
        side_each(step, "send")
        for part, (first, width) in enumerate(parts):
            lat_each(step, part, "recv")
            lat_each(step, part, "send")
            keep = step == STEPS - 2 and part > 0

            @pl.loop(first + 1, first + width + 1)
            def _(x):
                for place, y in enumerate((1, rows)):
                    later = advance(step, y, x)
                    other[y, x, inside] = later
                    if keep:
                        edge_ref[place, x - 1 - split] = later
                        pace_ref[place, x - 1 - split] = speed[y - 1, x - 1]

            lat_each(step + 1, part, "start")

            @pl.loop(first + 1, first + width + 1)
            def _(x):
                for y in range(2, rows):
                    other[y, x, inside] = advance(step, y, x)

        side_each(step + 1, "start")

    step = STEPS - 1
    now = fields[step % 2]
    side_each(step, "recv")

    @pl.loop(1, columns + 1)
    def _(x):
        for y in range(1, rows + 1):
            end_ref[y - 1, x - 1] = advance(step, y, x, low=y > 1, high=y < rows)

    side_each(step, "send")
    for part, (first, width) in enumerate(parts):
        lat_each(step, part, "recv")

        def finish():
            @pl.loop(first, first + width)
            def _(x):
                for row, halo in ((0, 0), (rows - 1, rows + 1)):
                    end_ref[row, x] = end_ref[row, x] + speed[row, x] * now[halo, x + 1, inside]

        finish() if part == 0 else pl.when(behind)(finish)
        lat_each(step, part, "send")


def tail_kernel(counts, pieces, end_ref, edge_ref, pace_ref, token_ref, last_ref, halo, send, recv):
    rows, columns = end_ref.shape[:2]
    width = edge_ref.shape[1]
    me, has = neighbours(counts)

    def lat_each(piece, act):
        span = pl.ds(pieces[piece], pieces[piece + 1] - pieces[piece])

        def copy_of(side, target):
            return pltpu.make_async_remote_copy(
                src_ref=edge_ref.at[side, span],
                dst_ref=halo.at[1 - side, span],
                send_sem=send.at[side, piece],
                recv_sem=recv.at[side, piece],
                device_id={"lat": target},
                device_id_type=MESH,
            )

        each_side(me, has, 0, act, copy_of)

    @pl.when(jnp.logical_not(late()))
    def _():
        greet(me, has, (0,))
        every = range(len(pieces) - 1)
        for piece in every:
            lat_each(piece, "start")
        for piece in every:
            lat_each(piece, "recv")
            for place, row in enumerate((0, rows - 1)):

                @pl.when(has[0][place])
                def _():
                    @pl.loop(pieces[piece], pieces[piece + 1])
                    def _(x):
                        last_ref[place, x] = end_ref[row, columns - width + x] + pace_ref[place, x] * halo[place, x]

                @pl.when(jnp.logical_not(has[0][place]))
                def _():
                    @pl.loop(pieces[piece], pieces[piece + 1])
                    def _(x):
                        last_ref[place, x] = end_ref[row, columns - width + x]

        for piece in every:
            lat_each(piece, "send")


def run(copies, there=None):
    def go():
        for copy in copies:
            copy.start()
        for copy in copies:
            copy.wait()

    go() if there is None else pl.when(there)(go)


def write_kernel(bounds, end_ref, out_ref, token_ref, sem):
    token_ref[...] = jnp.zeros_like(token_ref)
    rows, columns = out_ref.shape[:2]
    split = bounds[1]
    pieces = [(0, pl.ds(0, split)), (rows - 1, pl.ds(0, split))] + [(row, pl.ds(0, columns)) for row in range(1, rows - 1)]
    more = [(0, pl.ds(split, columns - split)), (rows - 1, pl.ds(split, columns - split))]
    copies = [
        pltpu.make_async_copy(end_ref.at[row, span], out_ref.at[row, span], sem.at[place])
        for place, (row, span) in enumerate(pieces + more)
    ]
    lagging = copies[len(pieces) :]

    @pl.when(late())
    def _():
        for copy in lagging:
            copy.start()

    run(copies[: len(pieces)])

    @pl.when(late())
    def _():
        for copy in lagging:
            copy.wait()


def patch_kernel(bounds, whole_ref, last_ref, out_ref, sem):
    rows, columns = out_ref.shape[:2]
    span = pl.ds(bounds[1], columns - bounds[1])
    run(
        [
            pltpu.make_async_copy(last_ref.at[place], out_ref.at[row, span], sem.at[place])
            for place, row in enumerate((0, rows - 1))
        ],
        jnp.logical_not(late()),
    )


def solution(mesh):
    counts = tuple(mesh.shape[axis] for axis in AXES)
    vmem, hbm = pl.BlockSpec(memory_space=pltpu.VMEM), pl.BlockSpec(memory_space=pltpu.HBM)
    dma = pltpu.SemaphoreType.DMA

    def shards(pressure, earlier, speed_square):
        rows, columns, depth, lanes = pressure.shape
        bounds = (0, columns - columns * TAIL // 64, columns)
        pieces = (0, bounds[2] - bounds[1] - columns * END // 64, bounds[2] - bounds[1])
        early_first = columns - columns * EARLY // 64
        parts = len(bounds) - 1
        edge = (2, columns - bounds[1], depth, lanes)
        field = pltpu.VMEM((rows + 2, columns + 2, depth + 2 * PAD, lanes), jnp.float32)
        end, edges, paces = pl.pallas_call(
            functools.partial(main_kernel, counts, bounds, early_first),
            out_shape=(pltpu.VMEM(pressure.shape, jnp.float32), pltpu.VMEM(edge, jnp.float32), pltpu.VMEM(edge, jnp.float32)),
            in_specs=[hbm] * 3,
            out_specs=(vmem,) * 3,
            scratch_shapes=[
                field,
                field,
                pltpu.VMEM(pressure.shape, jnp.float32),
                dma((6,)),
                dma((2, parts)),
                dma((2, 2, parts)),
                dma((2, 2)),
                dma((2, 2, 2)),
            ]
            + [pltpu.SemaphoreType.REGULAR] * 3,
            compiler_params=pltpu.CompilerParams(
                collective_id=0, has_side_effects=True, vmem_limit_bytes=44 * 2**20
            ),
        )(pressure, earlier, speed_square)
        out, token = pl.pallas_call(
            functools.partial(write_kernel, bounds),
            out_shape=(pltpu.HBM(pressure.shape, jnp.float32), pltpu.VMEM((8, 128), jnp.float32)),
            in_specs=[vmem],
            out_specs=(hbm, vmem),
            scratch_shapes=[dma((rows + 2,))],
            compiler_params=pltpu.CompilerParams(vmem_limit_bytes=2**20),
        )(end)
        last = pl.pallas_call(
            functools.partial(tail_kernel, counts, pieces),
            out_shape=pltpu.VMEM(edge, jnp.float32),
            in_specs=[vmem] * 4,
            out_specs=vmem,
            scratch_shapes=[
                pltpu.VMEM(edge, jnp.float32),
                dma((2, 2)),
                dma((2, 2)),
            ],
            compiler_params=pltpu.CompilerParams(
                collective_id=1, has_side_effects=True, vmem_limit_bytes=4 * 2**20
            ),
        )(end, edges, paces, token)
        return pl.pallas_call(
            functools.partial(patch_kernel, bounds),
            out_shape=pltpu.HBM(pressure.shape, jnp.float32),
            in_specs=[hbm, vmem],
            out_specs=hbm,
            input_output_aliases={0: 0},
            scratch_shapes=[dma((2,))],
            compiler_params=pltpu.CompilerParams(vmem_limit_bytes=2**20),
        )(out, last)

    spec = P("lat", "lon", "lev", None)
    return jax.shard_map(shards, mesh=mesh, in_specs=(spec, spec, spec), out_specs=spec, check_vma=False)
```

```python
import functools

import jax
import jax.numpy as jnp
from jax import lax
from jax.experimental import pallas as pl
from jax.experimental.pallas import tpu as pltpu
from jax.sharding import PartitionSpec as P

STEPS = 4
TAIL = 20
EARLY = 4
END = 2
PAD = 8
AXES = ("lat", "lon", "lev")
MESH = pl.DeviceIdType.MESH


def late():
    return lax.axis_index("lev") % 2 == 0


def neighbours(counts):
    me = [lax.axis_index(axis) for axis in AXES]
    return me, [(place > 0, place < count - 1) for place, count in zip(me, counts)]


def greet(me, has, dims):
    barrier = pltpu.get_barrier_semaphore()
    greeted = jnp.int32(0)
    for dim in dims:
        for side, shift in enumerate((-1, 1)):
            greeted = greeted + has[dim][side].astype(jnp.int32)

            @pl.when(has[dim][side])
            def _():
                pl.semaphore_signal(barrier, inc=1, device_id={AXES[dim]: me[dim] + shift}, device_id_type=MESH)

    pl.semaphore_wait(barrier, greeted)


def each_side(me, has, dim, act, copy_of, also=None, sides=(0, 1)):
    incoming = act == "recv"
    for side in sides:
        shift = (-1, 1)[side]
        there = has[dim][1 - side if incoming else side]
        if also is not None:
            there = jnp.logical_and(there, also)

        @pl.when(there)
        def _():
            copy = copy_of(side, me[dim] - shift if incoming else me[dim] + shift)
            if incoming:
                copy.wait_recv()
            elif act == "send":
                copy.wait_send()
            else:
                copy.start()


def main_kernel(
    counts,
    bounds,
    early_first,
    start_ref,
    earlier_ref,
    speed_ref,
    end_ref,
    edge_ref,
    pace_ref,
    even,
    odd,
    speed,
    load_sem,
    lat_send,
    lat_recv,
    side_send,
    side_recv,
    reply_sem,
    level_sem,
    beside_sem,
):
    rows, columns, depth, lanes = start_ref.shape
    fields = (even, odd)
    inside = pl.ds(PAD, depth)
    me, has = neighbours(counts)
    parts = [(first, after - first) for first, after in zip(bounds, bounds[1:])]
    split = bounds[1]

    early = [
        pltpu.make_async_copy(
            start_ref.at[plane, pl.ds(early_first, columns - early_first)],
            even.at[plane + 1, pl.ds(1 + early_first, columns - early_first), inside],
            load_sem.at[place],
        )
        for place, plane in enumerate((0, rows - 1))
    ]
    starts = [
        pltpu.make_async_copy(
            start_ref.at[:, pl.ds(0, early_first)],
            even.at[pl.ds(1, rows), pl.ds(1, early_first), inside],
            load_sem.at[2],
        )
    ]
    if rows > 2:
        starts.append(
            pltpu.make_async_copy(
                start_ref.at[pl.ds(1, rows - 2), pl.ds(early_first, columns - early_first)],
                even.at[pl.ds(2, rows - 2), pl.ds(1 + early_first, columns - early_first), inside],
                load_sem.at[3],
            )
        )
    loads = [
        pltpu.make_async_copy(earlier_ref, odd.at[pl.ds(1, rows), pl.ds(1, columns), inside], load_sem.at[4]),
        pltpu.make_async_copy(speed_ref, speed, load_sem.at[5]),
    ]
    behind = late()
    ahead = jnp.logical_not(behind)

    for load in early:
        load.start()

    @pl.when(behind)
    def _():
        for load in starts:
            load.start()

    low, high = has[0]
    bottom = jnp.logical_not(low)
    barrier = pltpu.get_barrier_semaphore()
    beside = sum(there.astype(jnp.int32) for dim in (1, 2) for there in has[dim])

    def tell_beside(sem):
        for dim in (1, 2):
            for side, shift in enumerate((-1, 1)):

                @pl.when(has[dim][side])
                def _():
                    pl.semaphore_signal(sem, inc=1, device_id={AXES[dim]: me[dim] + shift}, device_id_type=MESH)

    @pl.when(high)
    def _():
        pl.semaphore_signal(barrier, inc=1, device_id={"lat": me[0] + 1}, device_id_type=MESH)

    @pl.when(bottom)
    def _():
        tell_beside(barrier)

    @pl.when(low)
    def _():
        pl.semaphore_wait(barrier, 1)
        pl.semaphore_signal(reply_sem, inc=1, device_id={"lat": me[0] - 1}, device_id_type=MESH)

    def lat_piece(step, part, act, first, width, also=None, sides=(0, 1), held=True):
        field = fields[step % 2]

        def copy_of(side, target):
            if held:
                source = field.at[(1, rows)[side], pl.ds(first + 1, width), inside]
            else:
                source = start_ref.at[(0, rows - 1)[side], pl.ds(first, width)]
            return pltpu.make_async_remote_copy(
                src_ref=source,
                dst_ref=field.at[(rows + 1, 0)[side], pl.ds(first + 1, width), inside],
                send_sem=lat_send.at[side, part],
                recv_sem=lat_recv.at[step % 2, side, part],
                device_id={"lat": target},
                device_id_type=MESH,
            )

        each_side(me, has, 0, act, copy_of, also, sides)

    def lat_each(step, part, act):
        lat_piece(step, part, act, *parts[part], behind if step == STEPS - 1 and part > 0 else None)

    def lat_first(side):
        lat_piece(0, 1, "start", early_first, columns - early_first, ahead, (side,))
        lat_piece(0, 0, "start", 0, split, ahead, (side,), held=False)
        lat_piece(0, 1, "start", split, early_first - split, ahead, (side,), held=False)
        for part, piece in enumerate(parts):
            lat_piece(0, part, "start", *piece, behind, (side,))

    def side_each(step, act):
        field = fields[step % 2]
        for dim in (1, 2):

            def copy_of(side, target):
                if dim == 1:
                    if step == 0:
                        source = start_ref.at[:, (0, columns - 1)[side]]
                    else:
                        source = field.at[pl.ds(1, rows), (1, columns)[side], inside]
                    dest = field.at[pl.ds(1, rows), (columns + 1, 0)[side], inside]
                else:
                    if step == 0:
                        source = start_ref.at[:, :, pl.ds((0, depth - PAD)[side], PAD)]
                    else:
                        source = field.at[pl.ds(1, rows), pl.ds(1, columns), pl.ds((PAD, depth)[side], PAD)]
                    dest = field.at[pl.ds(1, rows), pl.ds(1, columns), pl.ds((PAD + depth, 0)[side], PAD)]
                return pltpu.make_async_remote_copy(
                    src_ref=source,
                    dst_ref=dest,
                    send_sem=side_send.at[dim - 1, side],
                    recv_sem=side_recv.at[step % 2, dim - 1, side],
                    device_id={AXES[dim]: target},
                    device_id_type=MESH,
                )

            each_side(me, has, dim, act, copy_of)

    for load in early:
        load.wait()

    @pl.when(behind)
    def _():
        for load in starts:
            load.wait()

    lat_first(0)

    @pl.when(high)
    def _():
        pl.semaphore_wait(reply_sem, 1)

    lat_first(1)

    @pl.when(ahead)
    def _():
        for load in starts:
            load.start()

    for load in loads:
        load.start()

    @pl.when(bottom)
    def _():
        pl.semaphore_wait(barrier, beside)

    @pl.when(low)
    def _():
        pl.semaphore_wait(level_sem, 1)

    @pl.when(high)
    def _():
        tell_beside(beside_sem)
        pl.semaphore_wait(beside_sem, beside)
        pl.semaphore_signal(level_sem, inc=1, device_id={"lat": me[0] + 1}, device_id_type=MESH)

    side_each(0, "start")

    for side in (0, 1):

        @pl.when(jnp.logical_not(has[0][side]))
        def _():
            @pl.loop(1, columns + 1)
            def _(x):
                for field in fields:
                    field[(0, rows + 1)[side], x, inside] = jnp.zeros((depth, lanes), jnp.float32)

        @pl.when(jnp.logical_not(has[1][side]))
        def _():
            for field in fields:
                for y in range(1, rows + 1):
                    field[y, (0, columns + 1)[side], inside] = jnp.zeros((depth, lanes), jnp.float32)

        @pl.when(jnp.logical_not(has[2][side]))
        def _():
            @pl.loop(1, columns + 1)
            def _(x):
                for field in fields:
                    for y in range(1, rows + 1):
                        field[y, x, pl.ds((0, PAD + depth)[side], PAD)] = jnp.zeros((PAD, lanes), jnp.float32)

    @pl.when(ahead)
    def _():
        for load in starts:
            load.wait()

    for load in loads:
        load.wait()

    def advance(step, y, x, low=True, high=True):
        now, other = fields[step % 2], fields[(step + 1) % 2]
        middle = now[y, x, inside]
        spread = now[y, x - 1, inside] + now[y, x + 1, inside]
        if low:
            spread += now[y - 1, x, inside]
        if high:
            spread += now[y + 1, x, inside]
        spread += now[y, x, pl.ds(PAD - 1, depth)] + now[y, x, pl.ds(PAD + 1, depth)] - 6.0 * middle
        return 2.0 * middle - other[y, x, inside] + speed[y - 1, x - 1] * spread

    for step in range(STEPS - 1):
        other = fields[(step + 1) % 2]
        side_each(step, "recv")
        side_each(step, "send")
        for part, (first, width) in enumerate(parts):
            lat_each(step, part, "recv")
            lat_each(step, part, "send")
            keep = step == STEPS - 2 and part > 0

            @pl.loop(first + 1, first + width + 1)
            def _(x):
                for place, y in enumerate((1, rows)):
                    later = advance(step, y, x)
                    other[y, x, inside] = later
                    if keep:
                        edge_ref[place, x - 1 - split] = later
                        pace_ref[place, x - 1 - split] = speed[y - 1, x - 1]

            lat_each(step + 1, part, "start")

            @pl.loop(first + 1, first + width + 1)
            def _(x):
                for y in range(2, rows):
                    other[y, x, inside] = advance(step, y, x)

        side_each(step + 1, "start")

    step = STEPS - 1
    now = fields[step % 2]
    side_each(step, "recv")

    @pl.loop(1, columns + 1)
    def _(x):
        for y in range(1, rows + 1):
            end_ref[y - 1, x - 1] = advance(step, y, x, low=y > 1, high=y < rows)

    side_each(step, "send")
    for part, (first, width) in enumerate(parts):
        lat_each(step, part, "recv")

        def finish():
            @pl.loop(first, first + width)
            def _(x):
                for row, halo in ((0, 0), (rows - 1, rows + 1)):
                    end_ref[row, x] = end_ref[row, x] + speed[row, x] * now[halo, x + 1, inside]

        finish() if part == 0 else pl.when(behind)(finish)
        lat_each(step, part, "send")


def tail_kernel(counts, pieces, end_ref, edge_ref, pace_ref, token_ref, last_ref, halo, send, recv):
    rows, columns = end_ref.shape[:2]
    width = edge_ref.shape[1]
    me, has = neighbours(counts)

    def lat_each(piece, act):
        span = pl.ds(pieces[piece], pieces[piece + 1] - pieces[piece])

        def copy_of(side, target):
            return pltpu.make_async_remote_copy(
                src_ref=edge_ref.at[side, span],
                dst_ref=halo.at[1 - side, span],
                send_sem=send.at[side, piece],
                recv_sem=recv.at[side, piece],
                device_id={"lat": target},
                device_id_type=MESH,
            )

        each_side(me, has, 0, act, copy_of)

    @pl.when(jnp.logical_not(late()))
    def _():
        greet(me, has, (0,))
        every = range(len(pieces) - 1)
        for piece in every:
            lat_each(piece, "start")
        for piece in every:
            lat_each(piece, "recv")
            for place, row in enumerate((0, rows - 1)):

                @pl.when(has[0][place])
                def _():
                    @pl.loop(pieces[piece], pieces[piece + 1])
                    def _(x):
                        last_ref[place, x] = end_ref[row, columns - width + x] + pace_ref[place, x] * halo[place, x]

        for piece in every:
            lat_each(piece, "send")


def run(copies):
    for act in ("start", "wait"):
        for copy, there in copies:
            pl.when(there)(getattr(copy, act))


def write_kernel(counts, bounds, end_ref, out_ref, token_ref, sem):
    token_ref[...] = jnp.zeros_like(token_ref)
    rows, columns = out_ref.shape[:2]
    split = bounds[1]
    _, has = neighbours(counts)
    pieces = [(row, pl.ds(0, columns), True) for row in range(1, rows - 1)]
    for place, row in enumerate((0, rows - 1)):
        final = jnp.logical_or(late(), jnp.logical_not(has[0][place]))
        pieces += [(row, pl.ds(0, split), True), (row, pl.ds(split, columns - split), final)]
    run(
        [
            (pltpu.make_async_copy(end_ref.at[row, span], out_ref.at[row, span], sem.at[place]), there)
            for place, (row, span, there) in enumerate(pieces)
        ]
    )


def patch_kernel(counts, bounds, whole_ref, last_ref, out_ref, sem):
    rows, columns = out_ref.shape[:2]
    span = pl.ds(bounds[1], columns - bounds[1])
    _, has = neighbours(counts)
    run(
        [
            (
                pltpu.make_async_copy(last_ref.at[place], out_ref.at[row, span], sem.at[place]),
                jnp.logical_and(jnp.logical_not(late()), has[0][place]),
            )
            for place, row in enumerate((0, rows - 1))
        ]
    )


def solution(mesh):
    counts = tuple(mesh.shape[axis] for axis in AXES)
    vmem, hbm = pl.BlockSpec(memory_space=pltpu.VMEM), pl.BlockSpec(memory_space=pltpu.HBM)
    dma = pltpu.SemaphoreType.DMA

    def shards(pressure, earlier, speed_square):
        rows, columns, depth, lanes = pressure.shape
        bounds = (0, columns - columns * TAIL // 64, columns)
        pieces = (0, bounds[2] - bounds[1] - columns * END // 64, bounds[2] - bounds[1])
        early_first = columns - columns * EARLY // 64
        parts = len(bounds) - 1
        edge = (2, columns - bounds[1], depth, lanes)
        field = pltpu.VMEM((rows + 2, columns + 2, depth + 2 * PAD, lanes), jnp.float32)
        end, edges, paces = pl.pallas_call(
            functools.partial(main_kernel, counts, bounds, early_first),
            out_shape=(pltpu.VMEM(pressure.shape, jnp.float32), pltpu.VMEM(edge, jnp.float32), pltpu.VMEM(edge, jnp.float32)),
            in_specs=[hbm] * 3,
            out_specs=(vmem,) * 3,
            scratch_shapes=[
                field,
                field,
                pltpu.VMEM(pressure.shape, jnp.float32),
                dma((6,)),
                dma((2, parts)),
                dma((2, 2, parts)),
                dma((2, 2)),
                dma((2, 2, 2)),
            ]
            + [pltpu.SemaphoreType.REGULAR] * 3,
            compiler_params=pltpu.CompilerParams(
                collective_id=0, has_side_effects=True, vmem_limit_bytes=44 * 2**20
            ),
        )(pressure, earlier, speed_square)
        out, token = pl.pallas_call(
            functools.partial(write_kernel, counts, bounds),
            out_shape=(pltpu.HBM(pressure.shape, jnp.float32), pltpu.VMEM((8, 128), jnp.float32)),
            in_specs=[vmem],
            out_specs=(hbm, vmem),
            scratch_shapes=[dma((rows + 2,))],
            compiler_params=pltpu.CompilerParams(vmem_limit_bytes=2**20),
        )(end)
        last = pl.pallas_call(
            functools.partial(tail_kernel, counts, pieces),
            out_shape=pltpu.VMEM(edge, jnp.float32),
            in_specs=[vmem] * 4,
            out_specs=vmem,
            scratch_shapes=[
                pltpu.VMEM(edge, jnp.float32),
                dma((2, 2)),
                dma((2, 2)),
            ],
            compiler_params=pltpu.CompilerParams(
                collective_id=1, has_side_effects=True, vmem_limit_bytes=4 * 2**20
            ),
        )(end, edges, paces, token)
        return pl.pallas_call(
            functools.partial(patch_kernel, counts, bounds),
            out_shape=pltpu.HBM(pressure.shape, jnp.float32),
            in_specs=[hbm, vmem],
            out_specs=hbm,
            input_output_aliases={0: 0},
            scratch_shapes=[dma((2,))],
            compiler_params=pltpu.CompilerParams(vmem_limit_bytes=2**20),
        )(out, last)

    spec = P("lat", "lon", "lev", None)
    return jax.shard_map(shards, mesh=mesh, in_specs=(spec, spec, spec), out_specs=spec, check_vma=False)
```

```python
import functools

import jax
import jax.numpy as jnp
from jax import lax
from jax.experimental import pallas as pl
from jax.experimental.pallas import tpu as pltpu
from jax.sharding import PartitionSpec as P

STEPS = 4
TAIL = 16
EARLY = 2
END = 2
PAD = 8
AXES = ("lat", "lon", "lev")
MESH = pl.DeviceIdType.MESH


def late():
    return lax.axis_index("lev") % 2 == 0


def neighbours(counts):
    me = [lax.axis_index(axis) for axis in AXES]
    return me, [(place > 0, place < count - 1) for place, count in zip(me, counts)]


def greet(me, has, dims):
    barrier = pltpu.get_barrier_semaphore()
    greeted = jnp.int32(0)
    for dim in dims:
        for side, shift in enumerate((-1, 1)):
            greeted = greeted + has[dim][side].astype(jnp.int32)

            @pl.when(has[dim][side])
            def _():
                pl.semaphore_signal(barrier, inc=1, device_id={AXES[dim]: me[dim] + shift}, device_id_type=MESH)

    pl.semaphore_wait(barrier, greeted)


def each_side(me, has, dim, act, copy_of, also=None, sides=(0, 1)):
    incoming = act == "recv"
    for side in sides:
        shift = (-1, 1)[side]
        there = has[dim][1 - side if incoming else side]
        if also is not None:
            there = jnp.logical_and(there, also)

        @pl.when(there)
        def _():
            copy = copy_of(side, me[dim] - shift if incoming else me[dim] + shift)
            if incoming:
                copy.wait_recv()
            elif act == "send":
                copy.wait_send()
            else:
                copy.start()


def main_kernel(
    counts,
    bounds,
    early_first,
    start_ref,
    earlier_ref,
    speed_ref,
    end_ref,
    edge_ref,
    pace_ref,
    even,
    odd,
    speed,
    load_sem,
    lat_send,
    lat_recv,
    side_send,
    side_recv,
    reply_sem,
    level_sem,
    beside_sem,
):
    rows, columns, depth, lanes = start_ref.shape
    fields = (even, odd)
    inside = pl.ds(PAD, depth)
    me, has = neighbours(counts)
    parts = [(first, after - first) for first, after in zip(bounds, bounds[1:])]
    split = bounds[1]

    early = [
        pltpu.make_async_copy(
            start_ref.at[plane, pl.ds(early_first, columns - early_first)],
            even.at[plane + 1, pl.ds(1 + early_first, columns - early_first), inside],
            load_sem.at[place],
        )
        for place, plane in enumerate((0, rows - 1))
    ]
    starts = [
        pltpu.make_async_copy(
            start_ref.at[:, pl.ds(0, early_first)],
            even.at[pl.ds(1, rows), pl.ds(1, early_first), inside],
            load_sem.at[2],
        )
    ]
    if rows > 2:
        starts.append(
            pltpu.make_async_copy(
                start_ref.at[pl.ds(1, rows - 2), pl.ds(early_first, columns - early_first)],
                even.at[pl.ds(2, rows - 2), pl.ds(1 + early_first, columns - early_first), inside],
                load_sem.at[3],
            )
        )
    loads = [
        pltpu.make_async_copy(earlier_ref, odd.at[pl.ds(1, rows), pl.ds(1, columns), inside], load_sem.at[4]),
        pltpu.make_async_copy(speed_ref, speed, load_sem.at[5]),
    ]
    behind = late()
    ahead = jnp.logical_not(behind)

    for load in early:
        load.start()

    @pl.when(behind)
    def _():
        for load in starts:
            load.start()

    low, high = has[0]
    bottom = jnp.logical_not(low)
    barrier = pltpu.get_barrier_semaphore()
    beside = sum(there.astype(jnp.int32) for dim in (1, 2) for there in has[dim])

    def tell_beside(sem):
        for dim in (1, 2):
            for side, shift in enumerate((-1, 1)):

                @pl.when(has[dim][side])
                def _():
                    pl.semaphore_signal(sem, inc=1, device_id={AXES[dim]: me[dim] + shift}, device_id_type=MESH)

    @pl.when(high)
    def _():
        pl.semaphore_signal(barrier, inc=1, device_id={"lat": me[0] + 1}, device_id_type=MESH)

    @pl.when(bottom)
    def _():
        tell_beside(barrier)

    @pl.when(low)
    def _():
        pl.semaphore_wait(barrier, 1)
        pl.semaphore_signal(reply_sem, inc=1, device_id={"lat": me[0] - 1}, device_id_type=MESH)

    def lat_piece(step, part, act, first, width, also=None, sides=(0, 1), held=True):
        field = fields[step % 2]

        def copy_of(side, target):
            if held:
                source = field.at[(1, rows)[side], pl.ds(first + 1, width), inside]
            else:
                source = start_ref.at[(0, rows - 1)[side], pl.ds(first, width)]
            return pltpu.make_async_remote_copy(
                src_ref=source,
                dst_ref=field.at[(rows + 1, 0)[side], pl.ds(first + 1, width), inside],
                send_sem=lat_send.at[side, part],
                recv_sem=lat_recv.at[step % 2, side, part],
                device_id={"lat": target},
                device_id_type=MESH,
            )

        each_side(me, has, 0, act, copy_of, also, sides)

    def lat_each(step, part, act):
        lat_piece(step, part, act, *parts[part], behind if step == STEPS - 1 and part > 0 else None)

    def lat_first(side):
        lat_piece(0, 1, "start", early_first, columns - early_first, ahead, (side,))
        lat_piece(0, 0, "start", 0, split, ahead, (side,), held=False)
        lat_piece(0, 1, "start", split, early_first - split, ahead, (side,), held=False)
        for part, piece in enumerate(parts):
            lat_piece(0, part, "start", *piece, behind, (side,))

    def side_each(step, act):
        field = fields[step % 2]
        for dim in (1, 2):

            def copy_of(side, target):
                if dim == 1:
                    if step == 0:
                        source = start_ref.at[:, (0, columns - 1)[side]]
                    else:
                        source = field.at[pl.ds(1, rows), (1, columns)[side], inside]
                    dest = field.at[pl.ds(1, rows), (columns + 1, 0)[side], inside]
                else:
                    if step == 0:
                        source = start_ref.at[:, :, pl.ds((0, depth - PAD)[side], PAD)]
                    else:
                        source = field.at[pl.ds(1, rows), pl.ds(1, columns), pl.ds((PAD, depth)[side], PAD)]
                    dest = field.at[pl.ds(1, rows), pl.ds(1, columns), pl.ds((PAD + depth, 0)[side], PAD)]
                return pltpu.make_async_remote_copy(
                    src_ref=source,
                    dst_ref=dest,
                    send_sem=side_send.at[dim - 1, side],
                    recv_sem=side_recv.at[step % 2, dim - 1, side],
                    device_id={AXES[dim]: target},
                    device_id_type=MESH,
                )

            each_side(me, has, dim, act, copy_of)

    for load in early:
        load.wait()

    @pl.when(behind)
    def _():
        for load in starts:
            load.wait()

    lat_first(0)

    @pl.when(high)
    def _():
        pl.semaphore_wait(reply_sem, 1)

    lat_first(1)

    @pl.when(ahead)
    def _():
        for load in starts:
            load.start()

    for load in loads:
        load.start()

    @pl.when(bottom)
    def _():
        pl.semaphore_wait(barrier, beside)

    @pl.when(low)
    def _():
        pl.semaphore_wait(level_sem, 1)

    @pl.when(high)
    def _():
        tell_beside(beside_sem)
        pl.semaphore_wait(beside_sem, beside)
        pl.semaphore_signal(level_sem, inc=1, device_id={"lat": me[0] + 1}, device_id_type=MESH)

    side_each(0, "start")

    for side in (0, 1):

        @pl.when(jnp.logical_not(has[0][side]))
        def _():
            @pl.loop(1, columns + 1)
            def _(x):
                for field in fields:
                    field[(0, rows + 1)[side], x, inside] = jnp.zeros((depth, lanes), jnp.float32)

        @pl.when(jnp.logical_not(has[1][side]))
        def _():
            for field in fields:
                for y in range(1, rows + 1):
                    field[y, (0, columns + 1)[side], inside] = jnp.zeros((depth, lanes), jnp.float32)

        @pl.when(jnp.logical_not(has[2][side]))
        def _():
            @pl.loop(1, columns + 1)
            def _(x):
                for field in fields:
                    for y in range(1, rows + 1):
                        field[y, x, pl.ds((0, PAD + depth)[side], PAD)] = jnp.zeros((PAD, lanes), jnp.float32)

    @pl.when(ahead)
    def _():
        for load in starts:
            load.wait()

    for load in loads:
        load.wait()

    def advance(step, y, x, low=True, high=True):
        now, other = fields[step % 2], fields[(step + 1) % 2]
        middle = now[y, x, inside]
        spread = now[y, x - 1, inside] + now[y, x + 1, inside]
        if low:
            spread += now[y - 1, x, inside]
        if high:
            spread += now[y + 1, x, inside]
        spread += now[y, x, pl.ds(PAD - 1, depth)] + now[y, x, pl.ds(PAD + 1, depth)] - 6.0 * middle
        return 2.0 * middle - other[y, x, inside] + speed[y - 1, x - 1] * spread

    for step in range(STEPS - 1):
        other = fields[(step + 1) % 2]
        side_each(step, "recv")
        side_each(step, "send")
        for part, (first, width) in enumerate(parts):
            lat_each(step, part, "recv")
            lat_each(step, part, "send")
            keep = step == STEPS - 2 and part > 0

            @pl.loop(first + 1, first + width + 1)
            def _(x):
                for place, y in enumerate((1, rows)):
                    later = advance(step, y, x)
                    other[y, x, inside] = later
                    if keep:
                        edge_ref[place, x - 1 - split] = later
                        pace_ref[place, x - 1 - split] = speed[y - 1, x - 1]

            @pl.loop(first + 1, first + width + 1)
            def _(x):
                for y in range(2, rows):
                    other[y, x, inside] = advance(step, y, x)

            lat_each(step + 1, part, "start")

        side_each(step + 1, "start")

    step = STEPS - 1
    now = fields[step % 2]
    side_each(step, "recv")

    @pl.loop(1, columns + 1)
    def _(x):
        for y in range(1, rows + 1):
            end_ref[y - 1, x - 1] = advance(step, y, x, low=y > 1, high=y < rows)

    side_each(step, "send")
    for part, (first, width) in enumerate(parts):
        lat_each(step, part, "recv")

        def finish():
            @pl.loop(first, first + width)
            def _(x):
                for row, halo in ((0, 0), (rows - 1, rows + 1)):
                    end_ref[row, x] = end_ref[row, x] + speed[row, x] * now[halo, x + 1, inside]

        finish() if part == 0 else pl.when(behind)(finish)
        lat_each(step, part, "send")


def tail_kernel(counts, pieces, end_ref, edge_ref, pace_ref, token_ref, last_ref, halo, send, recv):
    rows, columns = end_ref.shape[:2]
    width = edge_ref.shape[1]
    me, has = neighbours(counts)

    def lat_each(piece, act):
        span = pl.ds(pieces[piece], pieces[piece + 1] - pieces[piece])

        def copy_of(side, target):
            return pltpu.make_async_remote_copy(
                src_ref=edge_ref.at[side, span],
                dst_ref=halo.at[1 - side, span],
                send_sem=send.at[side, piece],
                recv_sem=recv.at[side, piece],
                device_id={"lat": target},
                device_id_type=MESH,
            )

        each_side(me, has, 0, act, copy_of)

    @pl.when(jnp.logical_not(late()))
    def _():
        greet(me, has, (0,))
        every = range(len(pieces) - 1)
        for piece in every:
            lat_each(piece, "start")
        for piece in every:
            lat_each(piece, "recv")
            for place, row in enumerate((0, rows - 1)):

                @pl.when(has[0][place])
                def _():
                    @pl.loop(pieces[piece], pieces[piece + 1])
                    def _(x):
                        last_ref[place, x] = end_ref[row, columns - width + x] + pace_ref[place, x] * halo[place, x]

        for piece in every:
            lat_each(piece, "send")


def run(copies):
    for act in ("start", "wait"):
        for copy, there in copies:
            pl.when(there)(getattr(copy, act))


def write_kernel(counts, bounds, end_ref, out_ref, token_ref, sem):
    token_ref[...] = jnp.zeros_like(token_ref)
    rows, columns = out_ref.shape[:2]
    split = bounds[1]
    _, has = neighbours(counts)
    pieces = [(row, pl.ds(0, columns), True) for row in range(1, rows - 1)]
    for place, row in enumerate((0, rows - 1)):
        final = jnp.logical_or(late(), jnp.logical_not(has[0][place]))
        pieces += [(row, pl.ds(0, split), True), (row, pl.ds(split, columns - split), final)]
    run(
        [
            (pltpu.make_async_copy(end_ref.at[row, span], out_ref.at[row, span], sem.at[place]), there)
            for place, (row, span, there) in enumerate(pieces)
        ]
    )


def patch_kernel(counts, bounds, whole_ref, last_ref, out_ref, sem):
    rows, columns = out_ref.shape[:2]
    span = pl.ds(bounds[1], columns - bounds[1])
    _, has = neighbours(counts)
    run(
        [
            (
                pltpu.make_async_copy(last_ref.at[place], out_ref.at[row, span], sem.at[place]),
                jnp.logical_and(jnp.logical_not(late()), has[0][place]),
            )
            for place, row in enumerate((0, rows - 1))
        ]
    )


def solution(mesh):
    counts = tuple(mesh.shape[axis] for axis in AXES)
    vmem, hbm = pl.BlockSpec(memory_space=pltpu.VMEM), pl.BlockSpec(memory_space=pltpu.HBM)
    dma = pltpu.SemaphoreType.DMA

    def shards(pressure, earlier, speed_square):
        rows, columns, depth, lanes = pressure.shape
        bounds = (0, columns - columns * TAIL // 64, columns)
        pieces = (0, bounds[2] - bounds[1] - columns * END // 64, bounds[2] - bounds[1])
        early_first = columns - columns * EARLY // 64
        parts = len(bounds) - 1
        edge = (2, columns - bounds[1], depth, lanes)
        field = pltpu.VMEM((rows + 2, columns + 2, depth + 2 * PAD, lanes), jnp.float32)
        end, edges, paces = pl.pallas_call(
            functools.partial(main_kernel, counts, bounds, early_first),
            out_shape=(pltpu.VMEM(pressure.shape, jnp.float32), pltpu.VMEM(edge, jnp.float32), pltpu.VMEM(edge, jnp.float32)),
            in_specs=[hbm] * 3,
            out_specs=(vmem,) * 3,
            scratch_shapes=[
                field,
                field,
                pltpu.VMEM(pressure.shape, jnp.float32),
                dma((6,)),
                dma((2, parts)),
                dma((2, 2, parts)),
                dma((2, 2)),
                dma((2, 2, 2)),
            ]
            + [pltpu.SemaphoreType.REGULAR] * 3,
            compiler_params=pltpu.CompilerParams(
                collective_id=0, has_side_effects=True, vmem_limit_bytes=44 * 2**20
            ),
        )(pressure, earlier, speed_square)
        out, token = pl.pallas_call(
            functools.partial(write_kernel, counts, bounds),
            out_shape=(pltpu.HBM(pressure.shape, jnp.float32), pltpu.VMEM((8, 128), jnp.float32)),
            in_specs=[vmem],
            out_specs=(hbm, vmem),
            scratch_shapes=[dma((rows + 2,))],
            compiler_params=pltpu.CompilerParams(vmem_limit_bytes=2**20),
        )(end)
        last = pl.pallas_call(
            functools.partial(tail_kernel, counts, pieces),
            out_shape=pltpu.VMEM(edge, jnp.float32),
            in_specs=[vmem] * 4,
            out_specs=vmem,
            scratch_shapes=[
                pltpu.VMEM(edge, jnp.float32),
                dma((2, 2)),
                dma((2, 2)),
            ],
            compiler_params=pltpu.CompilerParams(
                collective_id=1, has_side_effects=True, vmem_limit_bytes=4 * 2**20
            ),
        )(end, edges, paces, token)
        return pl.pallas_call(
            functools.partial(patch_kernel, counts, bounds),
            out_shape=pltpu.HBM(pressure.shape, jnp.float32),
            in_specs=[hbm, vmem],
            out_specs=hbm,
            input_output_aliases={0: 0},
            scratch_shapes=[dma((2,))],
            compiler_params=pltpu.CompilerParams(vmem_limit_bytes=2**20),
        )(out, last)

    spec = P("lat", "lon", "lev", None)
    return jax.shard_map(shards, mesh=mesh, in_specs=(spec, spec, spec), out_specs=spec, check_vma=False)
```

```python
import functools

import jax
import jax.numpy as jnp
from jax import lax
from jax.experimental import pallas as pl
from jax.experimental.pallas import tpu as pltpu
from jax.sharding import PartitionSpec as P

STEPS = 4
TAIL = 14
EARLY = 2
END = 1
PAD = 8
AXES = ("lat", "lon", "lev")
MESH = pl.DeviceIdType.MESH


def late():
    return lax.axis_index("lev") % 2 == 0


def neighbours(counts):
    me = [lax.axis_index(axis) for axis in AXES]
    return me, [(place > 0, place < count - 1) for place, count in zip(me, counts)]


def greet(me, has, dims):
    barrier = pltpu.get_barrier_semaphore()
    greeted = jnp.int32(0)
    for dim in dims:
        for side, shift in enumerate((-1, 1)):
            greeted = greeted + has[dim][side].astype(jnp.int32)

            @pl.when(has[dim][side])
            def _():
                pl.semaphore_signal(barrier, inc=1, device_id={AXES[dim]: me[dim] + shift}, device_id_type=MESH)

    pl.semaphore_wait(barrier, greeted)


def each_side(me, has, dim, act, copy_of, also=None, sides=(0, 1)):
    incoming = act == "recv"
    for side in sides:
        shift = (-1, 1)[side]
        there = has[dim][1 - side if incoming else side]
        if also is not None:
            there = jnp.logical_and(there, also)

        @pl.when(there)
        def _():
            copy = copy_of(side, me[dim] - shift if incoming else me[dim] + shift)
            if incoming:
                copy.wait_recv()
            elif act == "send":
                copy.wait_send()
            else:
                copy.start()


def main_kernel(
    counts,
    bounds,
    early_first,
    start_ref,
    earlier_ref,
    speed_ref,
    end_ref,
    edge_ref,
    pace_ref,
    even,
    odd,
    speed,
    load_sem,
    lat_send,
    lat_recv,
    side_send,
    side_recv,
    reply_sem,
    level_sem,
    beside_sem,
):
    rows, columns, depth, lanes = start_ref.shape
    fields = (even, odd)
    inside = pl.ds(PAD, depth)
    me, has = neighbours(counts)
    parts = [(first, after - first) for first, after in zip(bounds, bounds[1:])]
    split = bounds[1]

    early = [
        pltpu.make_async_copy(
            start_ref.at[plane, pl.ds(early_first, columns - early_first)],
            even.at[plane + 1, pl.ds(1 + early_first, columns - early_first), inside],
            load_sem.at[place],
        )
        for place, plane in enumerate((0, rows - 1))
    ]
    starts = [
        pltpu.make_async_copy(
            start_ref.at[:, pl.ds(0, early_first)],
            even.at[pl.ds(1, rows), pl.ds(1, early_first), inside],
            load_sem.at[2],
        )
    ]
    if rows > 2:
        starts.append(
            pltpu.make_async_copy(
                start_ref.at[pl.ds(1, rows - 2), pl.ds(early_first, columns - early_first)],
                even.at[pl.ds(2, rows - 2), pl.ds(1 + early_first, columns - early_first), inside],
                load_sem.at[3],
            )
        )
    loads = [
        pltpu.make_async_copy(earlier_ref, odd.at[pl.ds(1, rows), pl.ds(1, columns), inside], load_sem.at[0]),
        pltpu.make_async_copy(speed_ref, speed, load_sem.at[1]),
    ]
    behind = late()
    ahead = jnp.logical_not(behind)

    for load in early:
        load.start()

    @pl.when(behind)
    def _():
        for load in starts:
            load.start()

    low, high = has[0]
    bottom = jnp.logical_not(low)
    barrier = pltpu.get_barrier_semaphore()
    beside = sum(there.astype(jnp.int32) for dim in (1, 2) for there in has[dim])

    def tell_beside(sem):
        for dim in (1, 2):
            for side, shift in enumerate((-1, 1)):

                @pl.when(has[dim][side])
                def _():
                    pl.semaphore_signal(sem, inc=1, device_id={AXES[dim]: me[dim] + shift}, device_id_type=MESH)

    @pl.when(high)
    def _():
        pl.semaphore_signal(barrier, inc=1, device_id={"lat": me[0] + 1}, device_id_type=MESH)

    @pl.when(bottom)
    def _():
        tell_beside(barrier)

    @pl.when(low)
    def _():
        pl.semaphore_wait(barrier, 1)
        pl.semaphore_signal(reply_sem, inc=1, device_id={"lat": me[0] - 1}, device_id_type=MESH)

    def lat_piece(step, part, act, first, width, also=None, sides=(0, 1), held=True):
        field = fields[step % 2]

        def copy_of(side, target):
            if held:
                source = field.at[(1, rows)[side], pl.ds(first + 1, width), inside]
            else:
                source = start_ref.at[(0, rows - 1)[side], pl.ds(first, width)]
            return pltpu.make_async_remote_copy(
                src_ref=source,
                dst_ref=field.at[(rows + 1, 0)[side], pl.ds(first + 1, width), inside],
                send_sem=lat_send.at[side, part],
                recv_sem=lat_recv.at[step % 2, side, part],
                device_id={"lat": target},
                device_id_type=MESH,
            )

        each_side(me, has, 0, act, copy_of, also, sides)

    def lat_each(step, part, act):
        lat_piece(step, part, act, *parts[part], behind if step == STEPS - 1 and part > 0 else None)

    def lat_first(side):
        lat_piece(0, 1, "start", early_first, columns - early_first, ahead, (side,))
        lat_piece(0, 0, "start", 0, split, ahead, (side,), held=False)
        lat_piece(0, 1, "start", split, early_first - split, ahead, (side,), held=False)
        for part, piece in enumerate(parts):
            lat_piece(0, part, "start", *piece, behind, (side,))

    def side_each(step, act):
        field = fields[step % 2]
        for dim in (1, 2):

            def copy_of(side, target):
                if dim == 1:
                    if step == 0:
                        source = start_ref.at[:, (0, columns - 1)[side]]
                    else:
                        source = field.at[pl.ds(1, rows), (1, columns)[side], inside]
                    dest = field.at[pl.ds(1, rows), (columns + 1, 0)[side], inside]
                else:
                    if step == 0:
                        source = start_ref.at[:, :, pl.ds((0, depth - PAD)[side], PAD)]
                    else:
                        source = field.at[pl.ds(1, rows), pl.ds(1, columns), pl.ds((PAD, depth)[side], PAD)]
                    dest = field.at[pl.ds(1, rows), pl.ds(1, columns), pl.ds((PAD + depth, 0)[side], PAD)]
                return pltpu.make_async_remote_copy(
                    src_ref=source,
                    dst_ref=dest,
                    send_sem=side_send.at[dim - 1, side],
                    recv_sem=side_recv.at[step % 2, dim - 1, side],
                    device_id={AXES[dim]: target},
                    device_id_type=MESH,
                )

            each_side(me, has, dim, act, copy_of)

    for load in early:
        load.wait()

    @pl.when(behind)
    def _():
        for load in starts:
            load.wait()

    lat_first(0)

    @pl.when(high)
    def _():
        pl.semaphore_wait(reply_sem, 1)

    lat_first(1)

    @pl.when(ahead)
    def _():
        for load in starts:
            load.start()

    for load in loads:
        load.start()

    @pl.when(bottom)
    def _():
        pl.semaphore_wait(barrier, beside)

    @pl.when(low)
    def _():
        pl.semaphore_wait(level_sem, 1)

    @pl.when(high)
    def _():
        tell_beside(beside_sem)
        pl.semaphore_wait(beside_sem, beside)
        pl.semaphore_signal(level_sem, inc=1, device_id={"lat": me[0] + 1}, device_id_type=MESH)

    side_each(0, "start")

    for side in (0, 1):

        @pl.when(jnp.logical_not(has[0][side]))
        def _():
            @pl.loop(1, columns + 1)
            def _(x):
                for field in fields:
                    field[(0, rows + 1)[side], x, inside] = jnp.zeros((depth, lanes), jnp.float32)

        @pl.when(jnp.logical_not(has[1][side]))
        def _():
            for field in fields:
                for y in range(1, rows + 1):
                    field[y, (0, columns + 1)[side], inside] = jnp.zeros((depth, lanes), jnp.float32)

        @pl.when(jnp.logical_not(has[2][side]))
        def _():
            @pl.loop(1, columns + 1)
            def _(x):
                for field in fields:
                    for y in range(1, rows + 1):
                        field[y, x, pl.ds((0, PAD + depth)[side], PAD)] = jnp.zeros((PAD, lanes), jnp.float32)

    @pl.when(ahead)
    def _():
        for load in starts:
            load.wait()

    for load in loads:
        load.wait()

    def advance(step, y, x, low=True, high=True):
        now, other = fields[step % 2], fields[(step + 1) % 2]
        middle = now[y, x, inside]
        spread = now[y, x - 1, inside] + now[y, x + 1, inside]
        if low:
            spread += now[y - 1, x, inside]
        if high:
            spread += now[y + 1, x, inside]
        spread += now[y, x, pl.ds(PAD - 1, depth)] + now[y, x, pl.ds(PAD + 1, depth)] - 6.0 * middle
        return 2.0 * middle - other[y, x, inside] + speed[y - 1, x - 1] * spread

    for step in range(STEPS - 1):
        other = fields[(step + 1) % 2]
        side_each(step, "recv")
        side_each(step, "send")
        for part, (first, width) in enumerate(parts):
            lat_each(step, part, "recv")
            lat_each(step, part, "send")
            keep = step == STEPS - 2 and part > 0

            @pl.loop(first + 1, first + width + 1)
            def _(x):
                for place, y in enumerate((1, rows)):
                    later = advance(step, y, x)
                    other[y, x, inside] = later
                    if keep:
                        edge_ref[place, x - 1 - split] = later
                        pace_ref[place, x - 1 - split] = speed[y - 1, x - 1]

            @pl.loop(first + 1, first + width + 1)
            def _(x):
                for y in range(2, rows):
                    other[y, x, inside] = advance(step, y, x)

            lat_each(step + 1, part, "start")

        side_each(step + 1, "start")

    step = STEPS - 1
    now = fields[step % 2]
    side_each(step, "recv")

    @pl.loop(1, columns + 1)
    def _(x):
        for y in range(1, rows + 1):
            end_ref[y - 1, x - 1] = advance(step, y, x, low=y > 1, high=y < rows)

    side_each(step, "send")
    for part, (first, width) in enumerate(parts):
        lat_each(step, part, "recv")

        def finish():
            @pl.loop(first, first + width)
            def _(x):
                for row, halo in ((0, 0), (rows - 1, rows + 1)):
                    end_ref[row, x] = end_ref[row, x] + speed[row, x] * now[halo, x + 1, inside]

        finish() if part == 0 else pl.when(behind)(finish)
        lat_each(step, part, "send")


def tail_kernel(counts, pieces, end_ref, edge_ref, pace_ref, token_ref, last_ref, halo, send, recv):
    rows, columns = end_ref.shape[:2]
    width = edge_ref.shape[1]
    me, has = neighbours(counts)

    def lat_each(piece, act):
        span = pl.ds(pieces[piece], pieces[piece + 1] - pieces[piece])

        def copy_of(side, target):
            return pltpu.make_async_remote_copy(
                src_ref=edge_ref.at[side, span],
                dst_ref=halo.at[1 - side, span],
                send_sem=send.at[side, piece],
                recv_sem=recv.at[side, piece],
                device_id={"lat": target},
                device_id_type=MESH,
            )

        each_side(me, has, 0, act, copy_of)

    @pl.when(jnp.logical_not(late()))
    def _():
        greet(me, has, (0,))
        every = range(len(pieces) - 1)
        for piece in every:
            lat_each(piece, "start")
        for piece in every:
            lat_each(piece, "recv")
            for place, row in enumerate((0, rows - 1)):

                @pl.when(has[0][place])
                def _():
                    @pl.loop(pieces[piece], pieces[piece + 1])
                    def _(x):
                        last_ref[place, x] = end_ref[row, columns - width + x] + pace_ref[place, x] * halo[place, x]

        for piece in every:
            lat_each(piece, "send")


def run(copies):
    for act in ("start", "wait"):
        for copy, there in copies:
            pl.when(there)(getattr(copy, act))


def write_kernel(counts, bounds, end_ref, out_ref, token_ref, sem):
    token_ref[...] = jnp.zeros_like(token_ref)
    rows, columns = out_ref.shape[:2]
    split = bounds[1]
    _, has = neighbours(counts)
    pieces = [(row, pl.ds(0, columns), True) for row in range(1, rows - 1)]
    for place, row in enumerate((0, rows - 1)):
        final = jnp.logical_or(late(), jnp.logical_not(has[0][place]))
        pieces += [(row, pl.ds(0, split), True), (row, pl.ds(split, columns - split), final)]
    run(
        [
            (pltpu.make_async_copy(end_ref.at[row, span], out_ref.at[row, span], sem.at[place]), there)
            for place, (row, span, there) in enumerate(pieces)
        ]
    )


def patch_kernel(counts, bounds, whole_ref, last_ref, out_ref, sem):
    rows, columns = out_ref.shape[:2]
    span = pl.ds(bounds[1], columns - bounds[1])
    _, has = neighbours(counts)
    run(
        [
            (
                pltpu.make_async_copy(last_ref.at[place], out_ref.at[row, span], sem.at[place]),
                jnp.logical_and(jnp.logical_not(late()), has[0][place]),
            )
            for place, row in enumerate((0, rows - 1))
        ]
    )


def solution(mesh):
    counts = tuple(mesh.shape[axis] for axis in AXES)
    vmem, hbm = pl.BlockSpec(memory_space=pltpu.VMEM), pl.BlockSpec(memory_space=pltpu.HBM)
    dma = pltpu.SemaphoreType.DMA

    def shards(pressure, earlier, speed_square):
        rows, columns, depth, lanes = pressure.shape
        bounds = (0, columns - columns * TAIL // 64, columns)
        pieces = (0, bounds[2] - bounds[1] - columns * END // 64, bounds[2] - bounds[1])
        early_first = columns - columns * EARLY // 64
        parts = len(bounds) - 1
        edge = (2, columns - bounds[1], depth, lanes)
        field = pltpu.VMEM((rows + 2, columns + 2, depth + 2 * PAD, lanes), jnp.float32)
        end, edges, paces = pl.pallas_call(
            functools.partial(main_kernel, counts, bounds, early_first),
            out_shape=(pltpu.VMEM(pressure.shape, jnp.float32), pltpu.VMEM(edge, jnp.float32), pltpu.VMEM(edge, jnp.float32)),
            in_specs=[hbm] * 3,
            out_specs=(vmem,) * 3,
            scratch_shapes=[
                field,
                field,
                pltpu.VMEM(pressure.shape, jnp.float32),
                dma((4,)),
                dma((2, parts)),
                dma((2, 2, parts)),
                dma((2, 2)),
                dma((2, 2, 2)),
            ]
            + [pltpu.SemaphoreType.REGULAR] * 3,
            compiler_params=pltpu.CompilerParams(
                collective_id=0, has_side_effects=True, vmem_limit_bytes=44 * 2**20
            ),
        )(pressure, earlier, speed_square)
        out, token = pl.pallas_call(
            functools.partial(write_kernel, counts, bounds),
            out_shape=(pltpu.HBM(pressure.shape, jnp.float32), pltpu.VMEM((8, 128), jnp.float32)),
            in_specs=[vmem],
            out_specs=(hbm, vmem),
            scratch_shapes=[dma((rows + 2,))],
            compiler_params=pltpu.CompilerParams(vmem_limit_bytes=2**20),
        )(end)
        last = pl.pallas_call(
            functools.partial(tail_kernel, counts, pieces),
            out_shape=pltpu.VMEM(edge, jnp.float32),
            in_specs=[vmem] * 4,
            out_specs=vmem,
            scratch_shapes=[
                pltpu.VMEM(edge, jnp.float32),
                dma((2, 2)),
                dma((2, 2)),
            ],
            compiler_params=pltpu.CompilerParams(
                collective_id=1, has_side_effects=True, vmem_limit_bytes=4 * 2**20
            ),
        )(end, edges, paces, token)
        return pl.pallas_call(
            functools.partial(patch_kernel, counts, bounds),
            out_shape=pltpu.HBM(pressure.shape, jnp.float32),
            in_specs=[hbm, vmem],
            out_specs=hbm,
            input_output_aliases={0: 0},
            scratch_shapes=[dma((2,))],
            compiler_params=pltpu.CompilerParams(vmem_limit_bytes=2**20),
        )(out, last)

    spec = P("lat", "lon", "lev", None)
    return jax.shard_map(shards, mesh=mesh, in_specs=(spec, spec, spec), out_specs=spec, check_vma=False)
```

```python
import functools

import jax
import jax.numpy as jnp
from jax import lax
from jax.experimental import pallas as pl
from jax.experimental.pallas import tpu as pltpu
from jax.sharding import PartitionSpec as P

STEPS = 4
TAIL = 18
EARLY = 2
END = 2
PAD = 8
AXES = ("lat", "lon", "lev")
MESH = pl.DeviceIdType.MESH


def late():
    return lax.axis_index("lev") % 2 == 0


def neighbours(counts):
    me = [lax.axis_index(axis) for axis in AXES]
    return me, [(place > 0, place < count - 1) for place, count in zip(me, counts)]


def greet(me, has, dims):
    barrier = pltpu.get_barrier_semaphore()
    greeted = jnp.int32(0)
    for dim in dims:
        for side, shift in enumerate((-1, 1)):
            greeted = greeted + has[dim][side].astype(jnp.int32)

            @pl.when(has[dim][side])
            def _():
                pl.semaphore_signal(barrier, inc=1, device_id={AXES[dim]: me[dim] + shift}, device_id_type=MESH)

    pl.semaphore_wait(barrier, greeted)


def each_side(me, has, dim, act, copy_of, also=None, sides=(0, 1)):
    incoming = act == "recv"
    for side in sides:
        shift = (-1, 1)[side]
        there = has[dim][1 - side if incoming else side]
        if also is not None:
            there = jnp.logical_and(there, also)

        @pl.when(there)
        def _():
            copy = copy_of(side, me[dim] - shift if incoming else me[dim] + shift)
            if incoming:
                copy.wait_recv()
            elif act == "send":
                copy.wait_send()
            else:
                copy.start()


def main_kernel(
    counts,
    bounds,
    early_first,
    start_ref,
    earlier_ref,
    speed_ref,
    end_ref,
    edge_ref,
    pace_ref,
    even,
    odd,
    speed,
    load_sem,
    lat_send,
    lat_recv,
    side_send,
    side_recv,
    reply_sem,
    level_sem,
    beside_sem,
):
    rows, columns, depth, lanes = start_ref.shape
    fields = (even, odd)
    inside = pl.ds(PAD, depth)
    me, has = neighbours(counts)
    parts = [(first, after - first) for first, after in zip(bounds, bounds[1:])]
    split = bounds[1]

    early = [
        pltpu.make_async_copy(
            start_ref.at[plane, pl.ds(early_first, columns - early_first)],
            even.at[plane + 1, pl.ds(1 + early_first, columns - early_first), inside],
            load_sem.at[place],
        )
        for place, plane in enumerate((0, rows - 1))
    ]
    starts = [
        pltpu.make_async_copy(
            start_ref.at[:, pl.ds(0, early_first)],
            even.at[pl.ds(1, rows), pl.ds(1, early_first), inside],
            load_sem.at[2],
        )
    ]
    if rows > 2:
        starts.append(
            pltpu.make_async_copy(
                start_ref.at[pl.ds(1, rows - 2), pl.ds(early_first, columns - early_first)],
                even.at[pl.ds(2, rows - 2), pl.ds(1 + early_first, columns - early_first), inside],
                load_sem.at[3],
            )
        )
    loads = [
        pltpu.make_async_copy(earlier_ref, odd.at[pl.ds(1, rows), pl.ds(1, columns), inside], load_sem.at[0]),
        pltpu.make_async_copy(speed_ref, speed, load_sem.at[1]),
    ]
    behind = late()
    ahead = jnp.logical_not(behind)

    for load in early:
        load.start()

    @pl.when(behind)
    def _():
        for load in starts:
            load.start()

    low, high = has[0]
    bottom = jnp.logical_not(low)
    barrier = pltpu.get_barrier_semaphore()
    beside = sum(there.astype(jnp.int32) for dim in (1, 2) for there in has[dim])

    def tell_beside(sem):
        for dim in (1, 2):
            for side, shift in enumerate((-1, 1)):

                @pl.when(has[dim][side])
                def _():
                    pl.semaphore_signal(sem, inc=1, device_id={AXES[dim]: me[dim] + shift}, device_id_type=MESH)

    @pl.when(high)
    def _():
        pl.semaphore_signal(barrier, inc=1, device_id={"lat": me[0] + 1}, device_id_type=MESH)

    @pl.when(bottom)
    def _():
        tell_beside(barrier)

    @pl.when(low)
    def _():
        pl.semaphore_wait(barrier, 1)
        pl.semaphore_signal(reply_sem, inc=1, device_id={"lat": me[0] - 1}, device_id_type=MESH)

    def lat_piece(step, part, act, first, width, also=None, sides=(0, 1), held=True):
        field = fields[step % 2]

        def copy_of(side, target):
            if held:
                source = field.at[(1, rows)[side], pl.ds(first + 1, width), inside]
            else:
                source = start_ref.at[(0, rows - 1)[side], pl.ds(first, width)]
            return pltpu.make_async_remote_copy(
                src_ref=source,
                dst_ref=field.at[(rows + 1, 0)[side], pl.ds(first + 1, width), inside],
                send_sem=lat_send.at[side, part],
                recv_sem=lat_recv.at[step % 2, side, part],
                device_id={"lat": target},
                device_id_type=MESH,
            )

        each_side(me, has, 0, act, copy_of, also, sides)

    def lat_each(step, part, act):
        lat_piece(step, part, act, *parts[part], behind if step == STEPS - 1 and part > 0 else None)

    def lat_first(side):
        lat_piece(0, 1, "start", early_first, columns - early_first, ahead, (side,))
        lat_piece(0, 0, "start", 0, split, ahead, (side,), held=False)
        lat_piece(0, 1, "start", split, early_first - split, ahead, (side,), held=False)
        for part, piece in enumerate(parts):
            lat_piece(0, part, "start", *piece, behind, (side,))

    def side_each(step, act):
        field = fields[step % 2]
        for dim in (1, 2):

            def copy_of(side, target):
                if dim == 1:
                    if step == 0:
                        source = start_ref.at[:, (0, columns - 1)[side]]
                    else:
                        source = field.at[pl.ds(1, rows), (1, columns)[side], inside]
                    dest = field.at[pl.ds(1, rows), (columns + 1, 0)[side], inside]
                else:
                    if step == 0:
                        source = start_ref.at[:, :, pl.ds((0, depth - PAD)[side], PAD)]
                    else:
                        source = field.at[pl.ds(1, rows), pl.ds(1, columns), pl.ds((PAD, depth)[side], PAD)]
                    dest = field.at[pl.ds(1, rows), pl.ds(1, columns), pl.ds((PAD + depth, 0)[side], PAD)]
                return pltpu.make_async_remote_copy(
                    src_ref=source,
                    dst_ref=dest,
                    send_sem=side_send.at[dim - 1, side],
                    recv_sem=side_recv.at[step % 2, dim - 1, side],
                    device_id={AXES[dim]: target},
                    device_id_type=MESH,
                )

            each_side(me, has, dim, act, copy_of)

    for load in early:
        load.wait()

    @pl.when(behind)
    def _():
        for load in starts:
            load.wait()

    lat_first(0)

    @pl.when(high)
    def _():
        pl.semaphore_wait(reply_sem, 1)

    lat_first(1)

    @pl.when(ahead)
    def _():
        for load in starts:
            load.start()

    for load in loads:
        load.start()

    @pl.when(bottom)
    def _():
        pl.semaphore_wait(barrier, beside)

    @pl.when(low)
    def _():
        pl.semaphore_wait(level_sem, 1)

    @pl.when(high)
    def _():
        tell_beside(beside_sem)
        pl.semaphore_wait(beside_sem, beside)
        pl.semaphore_signal(level_sem, inc=1, device_id={"lat": me[0] + 1}, device_id_type=MESH)

    side_each(0, "start")

    for side in (0, 1):

        @pl.when(jnp.logical_not(has[0][side]))
        def _():
            @pl.loop(1, columns + 1)
            def _(x):
                for field in fields:
                    field[(0, rows + 1)[side], x, inside] = jnp.zeros((depth, lanes), jnp.float32)

        @pl.when(jnp.logical_not(has[1][side]))
        def _():
            for field in fields:
                for y in range(1, rows + 1):
                    field[y, (0, columns + 1)[side], inside] = jnp.zeros((depth, lanes), jnp.float32)

        @pl.when(jnp.logical_not(has[2][side]))
        def _():
            @pl.loop(1, columns + 1)
            def _(x):
                for field in fields:
                    for y in range(1, rows + 1):
                        field[y, x, pl.ds((0, PAD + depth)[side], PAD)] = jnp.zeros((PAD, lanes), jnp.float32)

    @pl.when(ahead)
    def _():
        for load in starts:
            load.wait()

    for load in loads:
        load.wait()

    def advance(step, y, x, low=True, high=True):
        now, other = fields[step % 2], fields[(step + 1) % 2]
        middle = now[y, x, inside]
        spread = now[y, x - 1, inside] + now[y, x + 1, inside]
        if low:
            spread += now[y - 1, x, inside]
        if high:
            spread += now[y + 1, x, inside]
        spread += now[y, x, pl.ds(PAD - 1, depth)] + now[y, x, pl.ds(PAD + 1, depth)] - 6.0 * middle
        return 2.0 * middle - other[y, x, inside] + speed[y - 1, x - 1] * spread

    for step in range(STEPS - 1):
        other = fields[(step + 1) % 2]
        side_each(step, "recv")
        side_each(step, "send")
        for part, (first, width) in enumerate(parts):
            lat_each(step, part, "recv")
            lat_each(step, part, "send")
            keep = step == STEPS - 2 and part > 0

            @pl.loop(first + 1, first + width + 1)
            def _(x):
                for place, y in enumerate((1, rows)):
                    later = advance(step, y, x)
                    other[y, x, inside] = later
                    if keep:
                        edge_ref[place, x - 1 - split] = later
                        pace_ref[place, x - 1 - split] = speed[y - 1, x - 1]

            @pl.loop(first + 1, first + width + 1)
            def _(x):
                for y in range(2, rows):
                    other[y, x, inside] = advance(step, y, x)

            lat_each(step + 1, part, "start")

        side_each(step + 1, "start")

    step = STEPS - 1
    now = fields[step % 2]
    side_each(step, "recv")

    @pl.loop(1, columns + 1)
    def _(x):
        for y in range(1, rows + 1):
            end_ref[y - 1, x - 1] = advance(step, y, x, low=y > 1, high=y < rows)

    side_each(step, "send")
    for part, (first, width) in enumerate(parts):
        lat_each(step, part, "recv")

        def finish():
            @pl.loop(first, first + width)
            def _(x):
                for row, halo in ((0, 0), (rows - 1, rows + 1)):
                    end_ref[row, x] = end_ref[row, x] + speed[row, x] * now[halo, x + 1, inside]

        finish() if part == 0 else pl.when(behind)(finish)
        lat_each(step, part, "send")


def tail_kernel(counts, pieces, end_ref, edge_ref, pace_ref, token_ref, last_ref, halo, send, recv):
    rows, columns = end_ref.shape[:2]
    width = edge_ref.shape[1]
    me, has = neighbours(counts)

    def lat_each(piece, act):
        span = pl.ds(pieces[piece], pieces[piece + 1] - pieces[piece])

        def copy_of(side, target):
            return pltpu.make_async_remote_copy(
                src_ref=edge_ref.at[side, span],
                dst_ref=halo.at[1 - side, span],
                send_sem=send.at[side, piece],
                recv_sem=recv.at[side, piece],
                device_id={"lat": target},
                device_id_type=MESH,
            )

        each_side(me, has, 0, act, copy_of)

    @pl.when(jnp.logical_not(late()))
    def _():
        greet(me, has, (0,))
        every = range(len(pieces) - 1)
        for piece in every:
            lat_each(piece, "start")
        for piece in every:
            lat_each(piece, "recv")
            for place, row in enumerate((0, rows - 1)):

                @pl.when(has[0][place])
                def _():
                    @pl.loop(pieces[piece], pieces[piece + 1])
                    def _(x):
                        last_ref[place, x] = end_ref[row, columns - width + x] + pace_ref[place, x] * halo[place, x]

        for piece in every:
            lat_each(piece, "send")


def run(copies):
    for act in ("start", "wait"):
        for copy, there in copies:
            pl.when(there)(getattr(copy, act))


def write_kernel(counts, bounds, end_ref, out_ref, token_ref, sem):
    token_ref[...] = jnp.zeros_like(token_ref)
    rows, columns = out_ref.shape[:2]
    split = bounds[1]
    _, has = neighbours(counts)
    pieces = [(row, pl.ds(0, columns), True) for row in range(1, rows - 1)]
    for place, row in enumerate((0, rows - 1)):
        final = jnp.logical_or(late(), jnp.logical_not(has[0][place]))
        pieces += [(row, pl.ds(0, split), True), (row, pl.ds(split, columns - split), final)]
    run(
        [
            (pltpu.make_async_copy(end_ref.at[row, span], out_ref.at[row, span], sem.at[place]), there)
            for place, (row, span, there) in enumerate(pieces)
        ]
    )


def patch_kernel(counts, bounds, whole_ref, last_ref, out_ref, sem):
    rows, columns = out_ref.shape[:2]
    span = pl.ds(bounds[1], columns - bounds[1])
    _, has = neighbours(counts)
    run(
        [
            (
                pltpu.make_async_copy(last_ref.at[place], out_ref.at[row, span], sem.at[place]),
                jnp.logical_and(jnp.logical_not(late()), has[0][place]),
            )
            for place, row in enumerate((0, rows - 1))
        ]
    )


def solution(mesh):
    counts = tuple(mesh.shape[axis] for axis in AXES)
    vmem, hbm = pl.BlockSpec(memory_space=pltpu.VMEM), pl.BlockSpec(memory_space=pltpu.HBM)
    dma = pltpu.SemaphoreType.DMA

    def shards(pressure, earlier, speed_square):
        rows, columns, depth, lanes = pressure.shape
        bounds = (0, columns - columns * TAIL // 64, columns)
        pieces = (0, bounds[2] - bounds[1] - columns * END // 64, bounds[2] - bounds[1])
        early_first = columns - columns * EARLY // 64
        parts = len(bounds) - 1
        edge = (2, columns - bounds[1], depth, lanes)
        field = pltpu.VMEM((rows + 2, columns + 2, depth + 2 * PAD, lanes), jnp.float32)
        end, edges, paces = pl.pallas_call(
            functools.partial(main_kernel, counts, bounds, early_first),
            out_shape=(pltpu.VMEM(pressure.shape, jnp.float32), pltpu.VMEM(edge, jnp.float32), pltpu.VMEM(edge, jnp.float32)),
            in_specs=[hbm] * 3,
            out_specs=(vmem,) * 3,
            scratch_shapes=[
                field,
                field,
                pltpu.VMEM(pressure.shape, jnp.float32),
                dma((4,)),
                dma((2, parts)),
                dma((2, 2, parts)),
                dma((2, 2)),
                dma((2, 2, 2)),
            ]
            + [pltpu.SemaphoreType.REGULAR] * 3,
            compiler_params=pltpu.CompilerParams(
                collective_id=0, has_side_effects=True, vmem_limit_bytes=44 * 2**20
            ),
        )(pressure, earlier, speed_square)
        out, token = pl.pallas_call(
            functools.partial(write_kernel, counts, bounds),
            out_shape=(pltpu.HBM(pressure.shape, jnp.float32), pltpu.VMEM((8, 128), jnp.float32)),
            in_specs=[vmem],
            out_specs=(hbm, vmem),
            scratch_shapes=[dma((rows + 2,))],
            compiler_params=pltpu.CompilerParams(vmem_limit_bytes=2**20),
        )(end)
        last = pl.pallas_call(
            functools.partial(tail_kernel, counts, pieces),
            out_shape=pltpu.VMEM(edge, jnp.float32),
            in_specs=[vmem] * 4,
            out_specs=vmem,
            scratch_shapes=[
                pltpu.VMEM(edge, jnp.float32),
                dma((2, 2)),
                dma((2, 2)),
            ],
            compiler_params=pltpu.CompilerParams(
                collective_id=1, has_side_effects=True, vmem_limit_bytes=4 * 2**20
            ),
        )(end, edges, paces, token)
        return pl.pallas_call(
            functools.partial(patch_kernel, counts, bounds),
            out_shape=pltpu.HBM(pressure.shape, jnp.float32),
            in_specs=[hbm, vmem],
            out_specs=hbm,
            input_output_aliases={0: 0},
            scratch_shapes=[dma((2,))],
            compiler_params=pltpu.CompilerParams(vmem_limit_bytes=2**20),
        )(out, last)

    spec = P("lat", "lon", "lev", None)
    return jax.shard_map(shards, mesh=mesh, in_specs=(spec, spec, spec), out_specs=spec, check_vma=False)
```
